512 devices in a mesh: row: 4 (over y), col: 16 (over z), trial: 8 (over x, core).
Axes of the slice: x: 4, y: 4, z: 16, core: 2. Of those that a mesh axis runs over, the one named last changes fastest.
Arguments:
- pair_rows: bfloat16 [3072, 384, 128], P(('trial', 'row'), 'col'), parts along dimension 0, may hold values from -6 to 6
- left_weight: bfloat16 [1024, 128], P('trial'), parts along dimension 0, may hold values from -0.5 to 0.5
- right_weight: bfloat16 [1024, 128], P('trial'), parts along dimension 0, may hold values from -0.5 to 0.5
- left_gate: bfloat16 [1024, 128], P('trial'), parts along dimension 0, may hold values from -0.5 to 0.5
- right_gate: bfloat16 [1024, 128], P('trial'), parts along dimension 0, may hold values from -0.5 to 0.5
- mid_gain: float32 [128], replicated, may hold values from 0.25 to 1.75
- out_weight: bfloat16 [1024, 128], P('trial'), parts along dimension 0, may hold values from -0.5 to 0.5
- out_gate: bfloat16 [1024, 128], P('trial'), parts along dimension 0, may hold values from -0.5 to 0.5
Outputs:
- pair_change: bfloat16 [3072, 384, 128], P(('trial', 'row'), 'col'), parts along dimension 0
The draws below stay inside these ranges and needn't reach their ends.
There are 8 independent parts, one for each index of `trial`. The reference program is written for one: setup_inputs(seed, part) draws one part's arguments, and reference() takes and returns one part's arrays. A program takes and returns all parts, laid end to end along the dimension named above; an argument that names none is the same for every part. Nothing has to cross between parts.
All inputs are finite; a program needn't handle non-finite values.
Results may differ from the reference program's by a relative error of at most 0.015.
Values may be sent and summed in bfloat16 or wider, within the bound.
A program may use at most 64 MiB of HBM per device.

```python
import jax
import jax.numpy as jnp
from jax import lax

RESIDUES = 384
PAIR_WIDTH = 128
MIX_WIDTH = 128


def shard_levels(stream_key, shape, split, least, top_value):
    def one(axis_at, blocks):
        draws = jax.random.uniform(jax.random.fold_in(jax.random.fold_in(stream_key, 6), axis_at), (blocks,), jnp.float32, least / len(split), top_value / len(split))
        return jnp.repeat(jnp.exp(draws), shape[axis_at] // blocks).reshape((-1,) + (1,) * (len(shape) - axis_at - 1))

    factor_of = one(*split[0])
    for cut in split[1:]:
        factor_of = factor_of * one(*cut)
    return factor_of


def normal_values(own_key, extent, spread, bound, cuts=(), dtype=jnp.bfloat16):
    values = spread * jax.random.normal(own_key, extent, jnp.float32)
    if cuts:
        values = values * shard_levels(own_key, extent, cuts, -0.22, 0.18)
    return jnp.clip(values, -bound, bound).astype(dtype)


def setup_inputs(seed: int = 0, part: int = 0) -> dict:
    key_of = jax.random.split(jax.random.key(seed), 9)
    own_keys = jax.random.split(jax.random.fold_in(key_of[8], part), 9)
    return {
        "pair_rows": normal_values(own_keys[0], (RESIDUES, RESIDUES, PAIR_WIDTH), 1.0, 6.0, ((0, 4), (1, 16))),
        "left_weight": normal_values(own_keys[1], (PAIR_WIDTH, MIX_WIDTH), PAIR_WIDTH ** -0.5, 0.5),
        "right_weight": normal_values(own_keys[2], (PAIR_WIDTH, MIX_WIDTH), PAIR_WIDTH ** -0.5, 0.5),
        "left_gate": normal_values(own_keys[3], (PAIR_WIDTH, MIX_WIDTH), PAIR_WIDTH ** -0.5, 0.5),
        "right_gate": normal_values(own_keys[4], (PAIR_WIDTH, MIX_WIDTH), PAIR_WIDTH ** -0.5, 0.5),
        "mid_gain": jnp.clip(1.0 + 0.15 * jax.random.normal(key_of[5], (MIX_WIDTH,), jnp.float32), 0.25, 1.75),
        "out_weight": normal_values(own_keys[6], (MIX_WIDTH, PAIR_WIDTH), MIX_WIDTH ** -0.5, 0.5),
        "out_gate": normal_values(own_keys[7], (PAIR_WIDTH, PAIR_WIDTH), PAIR_WIDTH ** -0.5, 0.5),
    }


def norm_channels(values, channel_gain):
    centred = values - lax.optimization_barrier(jnp.mean(values, axis=-1, keepdims=True))
    return centred * lax.rsqrt(lax.optimization_barrier(jnp.mean(centred * centred, axis=-1, keepdims=True)) + 1e-05) * channel_gain

def both_factors(pair_in, left_weight, right_weight, left_gate, right_gate):
    ready = pair_in
    left = jnp.einsum('ijc,cd->ijd', ready.astype(jnp.float32), left_weight.astype(jnp.float32))
    left = left * jax.nn.sigmoid(jnp.einsum('ijc,cd->ijd', ready.astype(jnp.float32), left_gate.astype(jnp.float32)))
    right = jnp.einsum('ijc,cd->ijd', ready.astype(jnp.float32), right_weight.astype(jnp.float32))
    right = right * jax.nn.sigmoid(jnp.einsum('ijc,cd->ijd', ready.astype(jnp.float32), right_gate.astype(jnp.float32)))
    return (ready, left.astype(jnp.bfloat16), right.astype(jnp.bfloat16))

def close_update(mixed, ready, mid_gain, out_weight, out_gate):
    scaled = norm_channels(mixed.astype(jnp.float32), mid_gain).astype(jnp.bfloat16)
    scaled = lax.optimization_barrier(scaled)
    gate = jax.nn.sigmoid(jnp.einsum('ijc,cd->ijd', ready.astype(jnp.float32), out_gate.astype(jnp.float32)))
    return (jnp.einsum('ijd,dc->ijc', scaled.astype(jnp.float32), out_weight.astype(jnp.float32)) * gate).astype(jnp.bfloat16)

def reference(pair_rows, left_weight, right_weight, left_gate, right_gate, mid_gain, out_weight, out_gate):
    ready, left, right = both_factors(pair_rows, left_weight, right_weight, left_gate, right_gate)
    left, right = lax.optimization_barrier((left, right))

    def one_channel(pair_of):
        return (jnp.dot(pair_of[0].T, pair_of[1], preferred_element_type=jnp.float32) * RESIDUES ** (-0.5)).astype(jnp.bfloat16)
    mixed = jnp.moveaxis(lax.map(one_channel, (jnp.moveaxis(left, -1, 0), jnp.moveaxis(right, -1, 0))), 0, -1)
    mixed = lax.optimization_barrier(mixed)
    return close_update(mixed, ready, mid_gain, out_weight, out_gate)
```

```python
import functools

import jax
import jax.numpy as jnp
from jax import lax
from jax.experimental import pallas as pl
from jax.experimental.pallas import tpu as pltpu
from jax.sharding import PartitionSpec as P

MESH = pl.DeviceIdType.MESH
F32, BF16 = jnp.float32, jnp.bfloat16
ROWS, COLS = 4, 16
LINES, WIDE, CH = 96, 24, 128
FAR = 7
CHUNK = 2 * WIDE
SUBS = ((0, 4), (4, 8), (8, 12), (12, 16))


def sigmoid(x):
    return 0.5 + 0.5 * jnp.tanh(0.5 * x)


def nt(a, b):
    return lax.dot_general(a, b, (((1,), (1,)), ((), ())), preferred_element_type=F32)


def kernel(
    x_ref, lw_ref, lg_ref, rw_ref, rg_ref, gain_ref, ow_ref, og_ref,
    o_ref,
    xf, wt, gb, fac, zs, yb, zb, lb, rb, lm, rm, cs, cb, es, ds, gt, stat,
    ysend, yrecv, zsend, zrecv, xsend, xrecv, csend, crecv, esend, erecv,
):
    y = lax.axis_index("row")
    z = lax.axis_index("col")

    def row_at(o):
        return lax.rem(y + o, ROWS)

    def col_at(s):
        return lax.rem(z + s + COLS, COLS)

    steps = [(s, way) for s in range(FAR, 0, -1) for way in (0, 1)]

    barrier = pltpu.get_barrier_semaphore()
    for o in range(1, ROWS):
        pl.semaphore_signal(barrier, inc=1, device_id={"row": row_at(o)}, device_id_type=MESH)
    for s, way in steps:
        pl.semaphore_signal(
            barrier, inc=1, device_id={"col": col_at(s if way == 0 else -s)}, device_id_type=MESH
        )

    def arc_of(t):
        s = FAR - t // 2
        way = t % 2
        return lax.rem(z + COLS + (1 - 2 * way) * s - way, COLS)

    xf[pl.ds(0, LINES * WIDE), :] = x_ref[...].astype(F32)
    xf[pl.ds(LINES * WIDE, 32 * WIDE), :] = jnp.zeros((32 * WIDE, CH), F32)
    for n, ref in enumerate((lw_ref, lg_ref, rw_ref, rg_ref)):
        wt[pl.ds(CH * n, CH), :] = ref[...].astype(F32).T.astype(BF16)
    gb[...] = jnp.broadcast_to(gain_ref[...], (CH, CH)).T

    def project(arr):
        @pl.loop(0, WIDE)
        def _(i):
            parts = []
            for b in range(4):
                block = lax.rem(b + y, 4)
                parts.append(xf[pl.ds(block * (32 * WIDE) + i, 32, stride=WIDE), :])
            xi = jnp.concatenate(parts, axis=0).astype(BF16)
            both = nt(wt[pl.ds(2 * CH * arr, 2 * CH), :], xi)
            fac[arr, pl.ds(i, CH, stride=WIDE), :] = both[:CH] * sigmoid(both[CH:])

    def y_copy(arr, sub, o):
        t0, t1 = SUBS[sub]
        dest = row_at(o)
        return pltpu.make_async_remote_copy(
            src_ref=zs.at[arr, dest, pl.ds(t0, t1 - t0)],
            dst_ref=yb.at[arr, y, pl.ds(t0, t1 - t0)],
            send_sem=ysend.at[arr, sub, o - 1],
            recv_sem=yrecv.at[arr, sub, o - 1],
            device_id={"row": dest},
            device_id_type=MESH,
        )

    def split_rows(arr, sub):
        t0, t1 = SUBS[sub]

        @pl.loop(t0, t1)
        def _(t):
            arc = arc_of(t)
            for q in range(ROWS):
                first = pl.multiple_of((32 * q + 2 * arc) * WIDE, 16)
                zs[arr, q, t] = fac[arr, pl.ds(first, CHUNK), :].astype(BF16)
            first = pl.multiple_of((32 * y + 2 * arc) * WIDE, 16)
            yb[arr, y, t] = fac[arr, pl.ds(first, CHUNK), :].astype(BF16)

    project(0)
    split_rows(0, 0)
    pl.semaphore_wait(barrier, ROWS - 1 + len(steps))
    for sub in range(len(SUBS)):
        if sub:
            split_rows(0, sub)
        for o in range(1, ROWS):
            y_copy(0, sub, o).start()
    project(1)
    for sub in range(len(SUBS)):
        split_rows(1, sub)
        for o in range(1, ROWS):
            y_copy(1, sub, o).start()

    def z_copy(arr, s, way):
        t = 2 * (FAR - s) + way
        dst = lb.at[way, z] if arr == 0 else rb.at[way, s]
        return pltpu.make_async_remote_copy(
            src_ref=zb.at[arr, t],
            dst_ref=dst,
            send_sem=zsend.at[arr, t],
            recv_sem=zrecv.at[arr, t],
            device_id={"col": col_at(s if way == 0 else -s)},
            device_id_type=MESH,
        )

    lane = lax.broadcasted_iota(jnp.int32, (CHUNK, CH), 1)

    def join(arr, t):
        a, b, c, d = (yb[arr, q, t].astype(F32) for q in range(ROWS))
        return jnp.concatenate(
            [
                jnp.where(lane < 96, a, b),
                jnp.where(lane < 64, b, c),
                jnp.where(lane < 32, c, d),
            ],
            axis=1,
        ).astype(BF16)

    for arr in (0, 1):
        for sub, (t0, t1) in enumerate(SUBS):
            for o in range(1, ROWS):
                y_copy(arr, sub, o).wait_recv()

            @pl.loop(t0, min(t1, 2 * FAR))
            def _(t):
                zb[arr, t] = join(arr, t)

            for t in range(max(t0, 2 * FAR), t1):
                way = t % 2
                if arr == 0:
                    lb[way, z] = join(arr, t)
                else:
                    rb[way, 0] = join(arr, t)
            for t in range(t0, min(t1, 2 * FAR)):
                z_copy(arr, FAR - t // 2, t % 2).start()

    @pl.loop(0, 6)
    def _(n):
        rows = pl.ds(pl.multiple_of(n * 384, 384), 384)
        g = jnp.dot(x_ref[rows, :], og_ref[...], preferred_element_type=F32)
        gt[rows, :] = sigmoid(g)

    def x_copy(s, way):
        src = col_at(-s if way == 0 else s)
        return pltpu.make_async_remote_copy(
            src_ref=lb.at[way, src],
            dst_ref=lb.at[1 - way, src],
            send_sem=xsend.at[way, s],
            recv_sem=xrecv.at[way, s],
            device_id={"col": col_at(1 if way == 0 else -1)},
            device_id_type=MESH,
        )

    for way in (0, 1):
        x_copy(0, way).start()
    for s, way in steps[::-1]:
        z_copy(0, s, way).wait_recv()
        x_copy(s, way).start()

    for s, way in steps[::-1]:
        z_copy(1, s, way).wait_recv()

    @pl.loop(0, 2)
    def _(way):
        for s in range(0, 8, 2):
            one, two = rb[way, s].astype(F32), rb[way, s + 1].astype(F32)
            for ph in (0, 1):
                cut = slice(WIDE * ph, WIDE * ph + WIDE)
                rm[way, ph, pl.ds(WIDE * s, CHUNK), :] = jnp.concatenate(
                    [one[cut], two[cut]], axis=0
                ).astype(BF16)

    for way in (0, 1):
        for s in range(8):
            x_copy(s, way).wait_recv()

    def c_copy(s, way):
        t = 2 * (FAR - s) + way
        return pltpu.make_async_remote_copy(
            src_ref=cs.at[t],
            dst_ref=cb.at[t],
            send_sem=csend.at[t],
            recv_sem=crecv.at[t],
            device_id={"col": col_at(-s if way == 0 else s)},
            device_id_type=MESH,
        )

    scale = (ROWS * LINES) ** -0.5
    for way in (0, 1):
        for q in range(ROWS):
            four = [lb[way, 4 * q + n].astype(F32) for n in range(4)]
            for ph in (0, 1):
                cut = slice(WIDE * ph, WIDE * ph + WIDE)
                lines = jnp.concatenate([f[cut] for f in four], axis=0).astype(BF16)
                for u in range(3):
                    lm[way, ph, pl.ds(128 * u + 32 * ((q + u) % 4), 32), :] = lines[
                        32 * u : 32 * u + 32
                    ]
        sums = [nt(rm[way, ph], lm[way, ph]) * scale for ph in (0, 1)]
        for s in range(FAR, -1, -1):
            cut = slice(WIDE * s, WIDE * s + WIDE)
            chunk = jnp.concatenate([sums[0][cut], sums[1][cut]], axis=0).astype(BF16)
            if s == 0:
                cb[2 * FAR + way] = chunk
            else:
                cs[2 * (FAR - s) + way] = chunk
        for s in range(FAR, 0, -1):
            c_copy(s, way).start()

    def e_copy(sub, o):
        t0, t1 = SUBS[sub]
        dest = row_at(o)
        return pltpu.make_async_remote_copy(
            src_ref=es.at[dest, pl.ds(t0, t1 - t0)],
            dst_ref=ds.at[y, pl.ds(t0, t1 - t0)],
            send_sem=esend.at[sub, o - 1],
            recv_sem=erecv.at[sub, o - 1],
            device_id={"row": dest},
            device_id_type=MESH,
        )

    strip = lane // 32

    for sub, (t0, t1) in enumerate(SUBS):
        for t in range(t0, min(t1, 2 * FAR)):
            c_copy(FAR - t // 2, t % 2).wait_recv()

        @pl.loop(t0, t1)
        def _(t):
            a, b, c = (cb[t, :, pl.ds(128 * u, 128)].astype(F32) for u in range(3))

            def quarter(q):
                return jnp.where(
                    strip == q, a, jnp.where(strip == lax.rem(q + 1, 4), b, c)
                ).astype(BF16)

            for q in range(ROWS):
                es[q, t] = quarter(q)
            ds[y, t] = quarter(y)

        for o in range(1, ROWS):
            e_copy(sub, o).start()

    mixed = fac.at[0]
    total = jnp.zeros((WIDE, CH), F32)
    for sub, (t0, t1) in enumerate(SUBS):
        for o in range(1, ROWS):
            e_copy(sub, o).wait_recv()

        def add(t, total):
            arc = arc_of(t)
            for q in range(ROWS):
                block = ds[q, t].astype(F32)
                first = pl.multiple_of((32 * q + 2 * arc) * WIDE, 16)
                mixed[pl.ds(first, CHUNK), :] = block
                total = total + block[:WIDE] + block[WIDE:]
            return total

        total = lax.fori_loop(t0, t1, add, total)
    mean = total * (1.0 / CH)

    def spread(n, total):
        for m in range(8):
            off = mixed[pl.ds(pl.multiple_of((8 * n + m) * WIDE, 8), WIDE), :] - mean
            total = total + off * off
        return total

    var = lax.fori_loop(0, CH // 8, spread, jnp.zeros((WIDE, CH), F32)) * (1.0 / CH)
    stat[0] = mean
    stat[1] = lax.rsqrt(var + 1e-05)

    out = fac.at[1]

    @pl.loop(0, WIDE)
    def _(j):
        block = mixed[pl.ds(j, CH, stride=WIDE), :]
        block = (block - stat[0, pl.ds(j, 1), :]) * stat[1, pl.ds(j, 1), :] * gb[...]
        change = jnp.dot(block.T.astype(BF16), ow_ref[...], preferred_element_type=F32)
        for b in range(4):
            u = lax.rem(b - y + 4, 4)
            out[pl.ds(u * (32 * WIDE) + j, 32, stride=WIDE), :] = change[32 * b : 32 * b + 32]

    @pl.loop(0, 6)
    def _(n):
        rows = pl.ds(pl.multiple_of(n * 384, 384), 384)
        o_ref[rows, :] = (out[rows, :] * gt[rows, :]).astype(BF16)

    for arr in (0, 1):
        for sub in range(len(SUBS)):
            for o in range(1, ROWS):
                y_copy(arr, sub, o).wait_send()
        for s, way in steps:
            z_copy(arr, s, way).wait_send()
    for way in (0, 1):
        for s in range(8):
            x_copy(s, way).wait_send()
    for s, way in steps:
        c_copy(s, way).wait_send()
    for sub in range(len(SUBS)):
        for o in range(1, ROWS):
            e_copy(sub, o).wait_send()


def per_device(
    pair_rows, left_weight, right_weight, left_gate, right_gate, mid_gain, out_weight, out_gate
):
    pixels = pair_rows.shape[0] * pair_rows.shape[1]
    dma = pltpu.SemaphoreType.DMA
    subs = len(SUBS)
    out = pl.pallas_call(
        kernel,
        out_shape=jax.ShapeDtypeStruct((pixels, CH), BF16),
        in_specs=[pl.BlockSpec(memory_space=pltpu.VMEM)] * 8,
        out_specs=pl.BlockSpec(memory_space=pltpu.VMEM),
        scratch_shapes=[
            pltpu.VMEM((128 * WIDE, CH), F32),
            pltpu.VMEM((4 * CH, CH), BF16),
            pltpu.VMEM((CH, CH), F32),
            pltpu.VMEM((2, CH * WIDE, CH), F32),
            pltpu.VMEM((2, ROWS, COLS, CHUNK, CH), BF16),
            pltpu.VMEM((2, ROWS, COLS, CHUNK, CH), BF16),
            pltpu.VMEM((2, COLS, CHUNK, 384), BF16),
            pltpu.VMEM((2, COLS, CHUNK, 384), BF16),
            pltpu.VMEM((2, 8, CHUNK, 384), BF16),
            pltpu.VMEM((2, 2, 384, 384), BF16),
            pltpu.VMEM((2, 2, 192, 384), BF16),
            pltpu.VMEM((COLS, CHUNK, 384), BF16),
            pltpu.VMEM((COLS, CHUNK, 384), BF16),
            pltpu.VMEM((ROWS, COLS, CHUNK, CH), BF16),
            pltpu.VMEM((ROWS, COLS, CHUNK, CH), BF16),
            pltpu.VMEM((pixels, CH), F32),
            pltpu.VMEM((2, WIDE, CH), F32),
            dma((2, subs, 3)), dma((2, subs, 3)),
            dma((2, 14)), dma((2, 14)),
            dma((2, 8)), dma((2, 8)),
            dma((14,)), dma((14,)),
            dma((subs, 3)), dma((subs, 3)),
        ],
        compiler_params=pltpu.CompilerParams(
            collective_id=0, has_side_effects=True, vmem_limit_bytes=48 * 1024 * 1024
        ),
    )(
        pair_rows.reshape(pixels, CH),
        left_weight, left_gate, right_weight, right_gate,
        mid_gain.reshape(1, CH), out_weight, out_gate,
    )
    return out.reshape(pair_rows.shape)


def solution(mesh):
    placed = (
        P(("trial", "row"), "col", None),
        P("trial", None),
        P("trial", None),
        P("trial", None),
        P("trial", None),
        P(),
        P("trial", None),
        P("trial", None),
    )
    return jax.shard_map(
        per_device,
        mesh=mesh,
        in_specs=placed,
        out_specs=P(("trial", "row"), "col", None),
        check_vma=False,
    )
```

```python
import functools

import jax
import jax.numpy as jnp
from jax import lax
from jax.experimental import pallas as pl
from jax.experimental.pallas import tpu as pltpu
from jax.sharding import PartitionSpec as P

MESH = pl.DeviceIdType.MESH
F32, BF16 = jnp.float32, jnp.bfloat16
ROWS, COLS = 4, 16
LINES, WIDE, CH = 96, 24, 128
FAR = 7
CHUNK = 2 * WIDE
YSUBS = (((0, 2), (2, 6), (6, 12), (12, 16)), ((12, 16), (8, 12), (4, 8), (0, 4)))
ESUBS = ((14, 16), (12, 14), (8, 12), (6, 8), (4, 6), (2, 4), (0, 2))


def sigmoid(x):
    return 0.5 + 0.5 * jnp.tanh(0.5 * x)


def nt(a, b):
    return lax.dot_general(a, b, (((1,), (1,)), ((), ())), preferred_element_type=F32)


def kernel(
    x_hbm, lw_hbm, lg_hbm, rw_hbm, rg_hbm, gain_hbm, ow_hbm, og_hbm,
    o_ref,
    x_ref, wraw, gain_ref, xf, wt, gb, facl, facr, zs, yb, zb, lb, rb, lm, rm, cs, cb, es, ds, gt, stat,
    insem, ysend, yrecv, zsend, zrecv, xsend, xrecv, csend, crecv, esend, erecv,
):
    y = lax.axis_index("row")
    z = lax.axis_index("col")

    def row_at(o):
        return lax.rem(y + o, ROWS)

    def col_at(s):
        return lax.rem(z + s + COLS, COLS)

    steps = [(s, way) for s in range(FAR, 0, -1) for way in (0, 1)]

    mats = (lw_hbm, lg_hbm, rw_hbm, rg_hbm, ow_hbm, og_hbm)
    loads = [pltpu.make_async_copy(x_hbm, x_ref, insem.at[0])]
    loads += [pltpu.make_async_copy(gain_hbm, gain_ref, insem.at[1])]
    loads += [pltpu.make_async_copy(m, wraw.at[n], insem.at[2 + n]) for n, m in enumerate(mats)]
    for load in loads:
        load.start()

    barrier = pltpu.get_barrier_semaphore()
    for o in range(1, ROWS):
        pl.semaphore_signal(barrier, inc=1, device_id={"row": row_at(o)}, device_id_type=MESH)
    for s, way in steps:
        pl.semaphore_signal(
            barrier, inc=1, device_id={"col": col_at(s if way == 0 else -s)}, device_id_type=MESH
        )

    def arc_of(t):
        s = FAR - t // 2
        way = t % 2
        return lax.rem(z + COLS + (1 - 2 * way) * s - way, COLS)

    facs = (facl, facr)

    xf[pl.ds(LINES * WIDE, 32 * WIDE), :] = jnp.zeros((32 * WIDE, CH), F32)
    for load in loads:
        load.wait()
    xf[pl.ds(0, LINES * WIDE), :] = x_ref[...].astype(F32)
    for n in range(4):
        wt[pl.ds(CH * n, CH), :] = wraw[n].astype(F32).T.astype(BF16)
    gb[...] = jnp.broadcast_to(gain_ref[...], (CH, CH)).T

    def project(arr):
        @pl.loop(0, WIDE // 2, unroll=3)
        def _(n):
            parts = []
            for i in (2 * n, 2 * n + 1):
                for b in range(4):
                    block = lax.rem(b + y, 4)
                    parts.append(xf[pl.ds(block * (32 * WIDE) + i, 32, stride=WIDE), :])
            xi = jnp.concatenate(parts, axis=0).astype(BF16)
            both = nt(wt[pl.ds(2 * CH * arr, 2 * CH), :], xi)
            value = both[:CH] * sigmoid(both[CH:])
            for m in range(2):
                facs[arr][pl.ds(2 * n + m, CH, stride=WIDE), :] = value[:, CH * m : CH * m + CH]

    def y_copy(arr, sub, o):
        t0, t1 = YSUBS[arr][sub]
        dest = row_at(o)
        return pltpu.make_async_remote_copy(
            src_ref=zs.at[arr, dest, pl.ds(t0, t1 - t0)],
            dst_ref=yb.at[arr, y, pl.ds(t0, t1 - t0)],
            send_sem=ysend.at[arr, sub, o - 1],
            recv_sem=yrecv.at[arr, sub, o - 1],
            device_id={"row": dest},
            device_id_type=MESH,
        )

    def split_rows(arr, sub):
        t0, t1 = YSUBS[arr][sub]

        @pl.loop(t0, t1)
        def _(t):
            arc = arc_of(t)
            for q in range(ROWS):
                first = pl.multiple_of((32 * q + 2 * arc) * WIDE, 16)
                zs[arr, q, t] = facs[arr][pl.ds(first, CHUNK), :].astype(BF16)
            first = pl.multiple_of((32 * y + 2 * arc) * WIDE, 16)
            yb[arr, y, t] = facs[arr][pl.ds(first, CHUNK), :].astype(BF16)

    def z_copy(arr, s, way):
        t = 2 * (FAR - s) + way
        dst = lb.at[way, z] if arr == 0 else rb.at[way, s]
        return pltpu.make_async_remote_copy(
            src_ref=zb.at[arr, t],
            dst_ref=dst,
            send_sem=zsend.at[arr, t],
            recv_sem=zrecv.at[arr, t],
            device_id={"col": col_at(s if way == 0 else -s)},
            device_id_type=MESH,
        )

    lane = lax.broadcasted_iota(jnp.int32, (CHUNK, CH), 1)

    def join(arr, t):
        a, b, c, d = (yb[arr, q, t].astype(F32) for q in range(ROWS))
        return jnp.concatenate(
            [
                jnp.where(lane < 96, a, b),
                jnp.where(lane < 64, b, c),
                jnp.where(lane < 32, c, d),
            ],
            axis=1,
        ).astype(BF16)

    def over_col(arr, sub):
        t0, t1 = YSUBS[arr][sub]
        for o in range(1, ROWS):
            y_copy(arr, sub, o).wait_recv()

        @pl.loop(t0, min(t1, 2 * FAR))
        def _(t):
            zb[arr, t] = join(arr, t)

        for t in range(max(t0, 2 * FAR), t1):
            way = t % 2
            if arr == 0:
                lb[way, z] = join(arr, t)
            else:
                rb[way, 0] = join(arr, t)
        sends = list(range(t0, min(t1, 2 * FAR)))
        for t in sends if arr == 0 else sends[::-1]:
            z_copy(arr, FAR - t // 2, t % 2).start()

    project(0)
    split_rows(0, 0)
    pl.semaphore_wait(barrier, ROWS - 1 + len(steps))
    for sub in range(4):
        if sub:
            split_rows(0, sub)
        for o in range(1, ROWS):
            y_copy(0, sub, o).start()
    project(1)
    over_col(0, 0)
    for sub in range(4):
        split_rows(1, sub)
        for o in range(1, ROWS):
            y_copy(1, sub, o).start()
        if sub < 3:
            over_col(0, sub + 1)
    over_col(1, 0)
    over_col(1, 1)

    @pl.loop(0, 6)
    def _(n):
        rows = pl.ds(pl.multiple_of(n * 384, 384), 384)
        g = jnp.dot(x_ref[rows, :], wraw[5], preferred_element_type=F32)
        gt[rows, :] = sigmoid(g)

    def x_copy(s, way):
        src = col_at(-s if way == 0 else s)
        return pltpu.make_async_remote_copy(
            src_ref=lb.at[way, src],
            dst_ref=lb.at[1 - way, src],
            send_sem=xsend.at[way, s],
            recv_sem=xrecv.at[way, s],
            device_id={"col": col_at(1 if way == 0 else -1)},
            device_id_type=MESH,
        )

    for way in (0, 1):
        x_copy(0, way).start()
    for s, way in steps[::-1]:
        z_copy(0, s, way).wait_recv()
        x_copy(s, way).start()

    over_col(1, 2)
    over_col(1, 3)

    def near_blocks(half):
        for s in range(4 * half, 4 * half + 4):
            if s:
                for way in (0, 1):
                    z_copy(1, s, way).wait_recv()
        for way in (0, 1):
            for s in range(4 * half, 4 * half + 4, 2):
                one, two = rb[way, s].astype(F32), rb[way, s + 1].astype(F32)
                for ph in (0, 1):
                    cut = slice(WIDE * ph, WIDE * ph + WIDE)
                    rm[way, ph, pl.ds(WIDE * s, CHUNK), :] = jnp.concatenate(
                        [one[cut], two[cut]], axis=0
                    ).astype(BF16)

    def c_copy(s, way):
        t = 2 * (FAR - s) + way
        return pltpu.make_async_remote_copy(
            src_ref=cs.at[t],
            dst_ref=cb.at[t],
            send_sem=csend.at[t],
            recv_sem=crecv.at[t],
            device_id={"col": col_at(-s if way == 0 else s)},
            device_id_type=MESH,
        )

    scale = (ROWS * LINES) ** -0.5
    near_blocks(0)
    for way in (0, 1):
        for s in range(8):
            x_copy(s, 1 - way).wait_recv()
        for q in range(ROWS):
            four = [lb[way, 4 * q + n].astype(F32) for n in range(4)]
            for ph in (0, 1):
                cut = slice(WIDE * ph, WIDE * ph + WIDE)
                lines = jnp.concatenate([f[cut] for f in four], axis=0).astype(BF16)
                for u in range(3):
                    lm[way, ph, pl.ds(128 * u + 32 * ((q + u) % 4), 32), :] = lines[
                        32 * u : 32 * u + 32
                    ]

    for half in (0, 1):
        if half:
            near_blocks(1)
        for way in (0, 1):
            rows = pl.ds(96 * half, 96)
            sums = [nt(rm[way, ph, rows, :], lm[way, ph]) * scale for ph in (0, 1)]
            for n in range(4):
                s = 4 * half + n
                cut = slice(WIDE * n, WIDE * n + WIDE)
                chunk = jnp.concatenate([sums[0][cut], sums[1][cut]], axis=0).astype(BF16)
                if s == 0:
                    cb[2 * FAR + way] = chunk
                else:
                    cs[2 * (FAR - s) + way] = chunk
        for s in range(max(4 * half, 1), 4 * half + 4):
            for way in (0, 1):
                c_copy(s, way).start()

    def e_copy(sub, o):
        t0, t1 = ESUBS[sub]
        dest = row_at(o)
        return pltpu.make_async_remote_copy(
            src_ref=es.at[dest, pl.ds(t0, t1 - t0)],
            dst_ref=ds.at[y, pl.ds(t0, t1 - t0)],
            send_sem=esend.at[sub, o - 1],
            recv_sem=erecv.at[sub, o - 1],
            device_id={"row": dest},
            device_id_type=MESH,
        )

    strip = lane // 32

    for sub, (t0, t1) in enumerate(ESUBS):
        for t in range(t0, min(t1, 2 * FAR)):
            c_copy(FAR - t // 2, t % 2).wait_recv()

        @pl.loop(t0, t1)
        def _(t):
            a, b, c = (cb[t, :, pl.ds(128 * u, 128)].astype(F32) for u in range(3))

            def quarter(q):
                return jnp.where(
                    strip == q, a, jnp.where(strip == lax.rem(q + 1, 4), b, c)
                ).astype(BF16)

            for q in range(ROWS):
                es[q, t] = quarter(q)
            ds[y, t] = quarter(y)

        for o in range(1, ROWS):
            e_copy(sub, o).start()

    mixed = facl
    total = jnp.zeros((WIDE, CH), F32)
    for sub, (t0, t1) in enumerate(ESUBS):
        for o in range(1, ROWS):
            e_copy(sub, o).wait_recv()

        def add(t, total):
            arc = arc_of(t)
            for q in range(ROWS):
                block = ds[q, t].astype(F32)
                first = pl.multiple_of((32 * q + 2 * arc) * WIDE, 16)
                mixed[pl.ds(first, CHUNK), :] = block
                total = total + block[:WIDE] + block[WIDE:]
            return total

        total = lax.fori_loop(t0, t1, add, total)
    mean = total * (1.0 / CH)

    def spread(n, total):
        for m in range(8):
            off = mixed[pl.ds(pl.multiple_of((8 * n + m) * WIDE, 8), WIDE), :] - mean
            total = total + off * off
        return total

    var = lax.fori_loop(0, CH // 8, spread, jnp.zeros((WIDE, CH), F32)) * (1.0 / CH)
    stat[0] = mean
    stat[1] = lax.rsqrt(var + 1e-05)

    out = facr

    @pl.loop(0, WIDE // 4)
    def _(n):
        scaled = []
        for j in range(4):
            block = mixed[pl.ds(4 * n + j, CH, stride=WIDE), :]
            block = (block - stat[0, pl.ds(4 * n + j, 1), :]) * stat[1, pl.ds(4 * n + j, 1), :] * gb[...]
            scaled.append(block.astype(BF16).T)
        change = jnp.dot(jnp.concatenate(scaled, axis=0), wraw[4], preferred_element_type=F32)
        for j in range(4):
            for b in range(4):
                u = lax.rem(b - y + 4, 4)
                out[pl.ds(u * (32 * WIDE) + 4 * n + j, 32, stride=WIDE), :] = change[
                    CH * j + 32 * b : CH * j + 32 * b + 32
                ]

    @pl.loop(0, 6)
    def _(n):
        rows = pl.ds(pl.multiple_of(n * 384, 384), 384)
        o_ref[rows, :] = (out[rows, :] * gt[rows, :]).astype(BF16)

    for arr in (0, 1):
        for sub in range(4):
            for o in range(1, ROWS):
                y_copy(arr, sub, o).wait_send()
        for s, way in steps:
            z_copy(arr, s, way).wait_send()
    for way in (0, 1):
        for s in range(8):
            x_copy(s, way).wait_send()
    for s, way in steps:
        c_copy(s, way).wait_send()
    for sub in range(len(ESUBS)):
        for o in range(1, ROWS):
            e_copy(sub, o).wait_send()


def per_device(
    pair_rows, left_weight, right_weight, left_gate, right_gate, mid_gain, out_weight, out_gate
):
    pixels = pair_rows.shape[0] * pair_rows.shape[1]
    dma = pltpu.SemaphoreType.DMA
    subs = len(ESUBS)
    out = pl.pallas_call(
        kernel,
        out_shape=jax.ShapeDtypeStruct((pixels, CH), BF16),
        in_specs=[pl.BlockSpec(memory_space=pltpu.HBM)] * 8,
        out_specs=pl.BlockSpec(memory_space=pltpu.VMEM),
        scratch_shapes=[
            pltpu.VMEM((pixels, CH), BF16),
            pltpu.VMEM((6, CH, CH), BF16),
            pltpu.VMEM((1, CH), F32),
            pltpu.VMEM((128 * WIDE, CH), F32),
            pltpu.VMEM((4 * CH, CH), BF16),
            pltpu.VMEM((CH, CH), F32),
            pltpu.VMEM((CH * WIDE, CH), F32),
            pltpu.VMEM((CH * WIDE, CH), F32),
            pltpu.VMEM((2, ROWS, COLS, CHUNK, CH), BF16),
            pltpu.VMEM((2, ROWS, COLS, CHUNK, CH), BF16),
            pltpu.VMEM((2, COLS, CHUNK, 384), BF16),
            pltpu.VMEM((2, COLS, CHUNK, 384), BF16),
            pltpu.VMEM((2, 8, CHUNK, 384), BF16),
            pltpu.VMEM((2, 2, 384, 384), BF16),
            pltpu.VMEM((2, 2, 192, 384), BF16),
            pltpu.VMEM((COLS, CHUNK, 384), BF16),
            pltpu.VMEM((COLS, CHUNK, 384), BF16),
            pltpu.VMEM((ROWS, COLS, CHUNK, CH), BF16),
            pltpu.VMEM((ROWS, COLS, CHUNK, CH), BF16),
            pltpu.VMEM((pixels, CH), F32),
            pltpu.VMEM((2, WIDE, CH), F32),
            dma((8,)),
            dma((2, 4, 3)), dma((2, 4, 3)),
            dma((2, 14)), dma((2, 14)),
            dma((2, 8)), dma((2, 8)),
            dma((14,)), dma((14,)),
            dma((subs, 3)), dma((subs, 3)),
        ],
        compiler_params=pltpu.CompilerParams(
            collective_id=0, has_side_effects=True, vmem_limit_bytes=67043328
        ),
    )(
        pair_rows.reshape(pixels, CH),
        left_weight, left_gate, right_weight, right_gate,
        mid_gain.reshape(1, CH), out_weight, out_gate,
    )
    return out.reshape(pair_rows.shape)


def solution(mesh):
    placed = (
        P(("trial", "row"), "col", None),
        P("trial", None),
        P("trial", None),
        P("trial", None),
        P("trial", None),
        P(),
        P("trial", None),
        P("trial", None),
    )
    return jax.shard_map(
        per_device,
        mesh=mesh,
        in_specs=placed,
        out_specs=P(("trial", "row"), "col", None),
        check_vma=False,
    )
```

```python
import functools

import jax
import jax.numpy as jnp
from jax import lax
from jax.experimental import pallas as pl
from jax.experimental.pallas import tpu as pltpu
from jax.sharding import PartitionSpec as P

MESH = pl.DeviceIdType.MESH
F32, BF16 = jnp.float32, jnp.bfloat16
ROWS, COLS = 4, 16
LINES, WIDE, CH = 96, 24, 128
TEAM = 4
FAR = (COLS - TEAM) // 2
CHUNK = 2 * WIDE
if TEAM == 4:
    YSUBS = (((0, 2), (2, 6), (6, 12), (12, 16)), ((12, 16), (8, 12), (4, 8), (2, 4), (0, 2)))
    ESUBS = ((12, 16), (10, 12), (6, 10), (4, 6), (2, 4), (0, 2))
else:
    YSUBS = (((0, 2), (2, 6), (6, 14), (14, 16)), ((14, 16), (8, 14), (4, 8), (2, 4), (0, 2)))
    ESUBS = ((14, 16), (12, 14), (8, 12), (6, 8), (4, 6), (2, 4), (0, 2))


def sigmoid(x):
    return 0.5 + 0.5 * jnp.tanh(0.5 * x)


def nt(a, b):
    return lax.dot_general(a, b, (((1,), (1,)), ((), ())), preferred_element_type=F32)


def kernel(
    x_hbm, lw_hbm, lg_hbm, rw_hbm, rg_hbm, gain_hbm, ow_hbm, og_hbm,
    o_ref,
    x_ref, wraw, gain_ref, xf, xr, wf, wt, gb, facl, facr, fac0, zs, yb, zb, lb, rb, ri, lm, rm,
    cs, cb, es, ds, gt, stat,
    insem, ysend, yrecv, zsend, zrecv, xsend, xrecv, csend, crecv, esend, erecv,
):
    y = lax.axis_index("row")
    z = lax.axis_index("col")

    def row_at(o):
        return lax.rem(y + o, ROWS)

    def col_at(s):
        return lax.rem(z + s + COLS, COLS)

    steps = [(s, way) for s in range(FAR, 0, -1) for way in (0, 1)]

    mats = (lw_hbm, lg_hbm, rw_hbm, rg_hbm, ow_hbm, og_hbm)
    loads = [pltpu.make_async_copy(m, wraw.at[n], insem.at[n]) for n, m in enumerate(mats)]
    loads += [pltpu.make_async_copy(gain_hbm, gain_ref, insem.at[6])]
    third = LINES * WIDE // 3
    loads += [
        pltpu.make_async_copy(
            x_hbm.at[pl.ds(third * n, third)], x_ref.at[pl.ds(third * n, third)], insem.at[7 + n]
        )
        for n in range(3)
    ]
    for load in loads:
        load.start()

    barrier = pltpu.get_barrier_semaphore()
    for o in range(1, ROWS):
        pl.semaphore_signal(barrier, inc=1, device_id={"row": row_at(o)}, device_id_type=MESH)
    for s, way in steps:
        pl.semaphore_signal(
            barrier, inc=1, device_id={"col": col_at(s if way == 0 else -s)}, device_id_type=MESH
        )

    def team_of(t, own):
        if own:
            return lax.rem(z + COLS - (t - 2 * FAR), COLS)
        s = FAR - t // 2
        way = t % 2
        return lax.rem(z + COLS + (1 - 2 * way) * s - (TEAM - 1) * way, COLS)

    facs = (facl, facr)

    xf[pl.ds(LINES * WIDE, 32 * WIDE), :] = jnp.zeros((32 * WIDE, CH), F32)
    for load in loads[:7]:
        load.wait()
    for n in range(4):
        turned = wraw[n].astype(F32).T
        if n < 2:
            wf[pl.ds(CH * n, CH), :] = turned
        wt[pl.ds(CH * n, CH), :] = turned.astype(BF16)
    gb[...] = jnp.broadcast_to(gain_ref[...], (CH, CH)).T
    picks = []
    for n in range(2):
        for t in range(2):
            for ph in range(2):
                picks.append(wf[pl.ds(CH * n + 2 * team_of(t, False) + ph, ROWS, stride=32), :])
    first_w = jnp.concatenate(picks, axis=0).astype(BF16)
    for n in range(3):
        loads[7 + n].wait()
        xf[pl.ds(third * n, third), :] = x_ref[pl.ds(third * n, third), :].astype(F32)

    @pl.loop(0, WIDE // 2, unroll=3)
    def _(n):
        parts = []
        for i in (2 * n, 2 * n + 1):
            for b in range(4):
                block = lax.rem(b + y, 4)
                parts.append(xf[pl.ds(block * (32 * WIDE) + i, 32, stride=WIDE), :])
        xi = jnp.concatenate(parts, axis=0).astype(BF16)
        xr[pl.ds(pl.multiple_of(2 * CH * n, 2 * CH), 2 * CH), :] = xi
        both = nt(first_w, xi)
        value = both[:16] * sigmoid(both[16:])
        for m in range(2):
            fac0[pl.ds(2 * n + m, 16, stride=WIDE), :] = value[:, CH * m : CH * m + CH]

    def project(arr):
        @pl.loop(0, WIDE // 2, unroll=3)
        def _(n):
            xi = xr[pl.ds(pl.multiple_of(2 * CH * n, 2 * CH), 2 * CH), :]
            both = nt(wt[pl.ds(2 * CH * arr, 2 * CH), :], xi)
            value = both[:CH] * sigmoid(both[CH:])
            for m in range(2):
                facs[arr][pl.ds(2 * n + m, CH, stride=WIDE), :] = value[:, CH * m : CH * m + CH]

    def y_copy(arr, sub, o):
        t0, t1 = YSUBS[arr][sub]
        dest = row_at(o)
        return pltpu.make_async_remote_copy(
            src_ref=zs.at[arr, dest, pl.ds(t0, t1 - t0)],
            dst_ref=yb.at[arr, y, pl.ds(t0, t1 - t0)],
            send_sem=ysend.at[arr, sub, o - 1],
            recv_sem=yrecv.at[arr, sub, o - 1],
            device_id={"row": dest},
            device_id_type=MESH,
        )

    def over_row(arr, sub):
        t0, t1 = YSUBS[arr][sub]

        @pl.loop(t0, t1)
        def _(t):
            team = team_of(t, t0 >= 2 * FAR)
            for q in range(ROWS):
                first = pl.multiple_of((32 * q + 2 * team) * WIDE, 16)
                zs[arr, q, t] = facs[arr][pl.ds(first, CHUNK), :].astype(BF16)
            first = pl.multiple_of((32 * y + 2 * team) * WIDE, 16)
            yb[arr, y, t] = facs[arr][pl.ds(first, CHUNK), :].astype(BF16)

        for o in range(1, ROWS):
            y_copy(arr, sub, o).start()

    def z_copy(arr, s, way):
        t = 2 * (FAR - s) + way
        dst = lb.at[(TEAM - 1) * way, z] if arr == 0 else rb.at[way, s]
        return pltpu.make_async_remote_copy(
            src_ref=zb.at[arr, t],
            dst_ref=dst,
            send_sem=zsend.at[arr, t],
            recv_sem=zrecv.at[arr, t],
            device_id={"col": col_at(s if way == 0 else -s)},
            device_id_type=MESH,
        )

    lane = lax.broadcasted_iota(jnp.int32, (CHUNK, CH), 1)

    def join(arr, t):
        a, b, c, d = (yb[arr, q, t].astype(F32) for q in range(ROWS))
        return jnp.concatenate(
            [
                jnp.where(lane < 96, a, b),
                jnp.where(lane < 64, b, c),
                jnp.where(lane < 32, c, d),
            ],
            axis=1,
        ).astype(BF16)

    def over_col(arr, sub):
        t0, t1 = YSUBS[arr][sub]
        for o in range(1, ROWS):
            y_copy(arr, sub, o).wait_recv()
        if t0 >= 2 * FAR:
            for e in range(TEAM):
                if arr == 0:
                    lb[e, z] = join(arr, t0 + e)
                elif e in (0, TEAM - 1):
                    rb[e // (TEAM - 1), 0] = join(arr, t0 + e)
                else:
                    ri[e - 1] = join(arr, t0 + e)
            return

        @pl.loop(t0, t1)
        def _(t):
            zb[arr, t] = join(arr, t)

        sends = list(range(t0, t1))
        for t in sends if arr == 0 else sends[::-1]:
            z_copy(arr, FAR - t // 2, t % 2).start()

    def x_copy(way, r, s):
        src = col_at(-s if way == 0 else s)
        e = r if way == 0 else TEAM - 1 - r
        return pltpu.make_async_remote_copy(
            src_ref=lb.at[e, src],
            dst_ref=lb.at[e + 1 - 2 * way, src],
            send_sem=xsend.at[way, r, s],
            recv_sem=xrecv.at[way, r, s],
            device_id={"col": col_at(1 if way == 0 else -1)},
            device_id_type=MESH,
        )

    def gates():
        @pl.loop(0, 6)
        def _(n):
            rows = pl.ds(pl.multiple_of(n * 384, 384), 384)
            g = jnp.dot(x_ref[rows, :], wraw[5], preferred_element_type=F32)
            gt[rows, :] = sigmoid(g)

    for t in range(2):
        for q in range(ROWS):
            rows = [((2 * t + ph) * ROWS + q) * WIDE for ph in range(2)]
            zs[0, q, t] = jnp.concatenate(
                [fac0[pl.ds(first, WIDE), :] for first in rows], axis=0
            ).astype(BF16)
        rows = [pl.multiple_of(((2 * t + ph) * ROWS + y) * WIDE, 8) for ph in range(2)]
        yb[0, y, t] = jnp.concatenate(
            [fac0[pl.ds(first, WIDE), :] for first in rows], axis=0
        ).astype(BF16)
    pl.semaphore_wait(barrier, ROWS - 1 + len(steps))
    for o in range(1, ROWS):
        y_copy(0, 0, o).start()

    project(0)
    over_row(0, 1)
    over_row(0, 2)
    over_col(0, 0)
    over_row(0, 3)
    project(1)
    over_col(0, 1)
    over_row(1, 0)
    over_row(1, 1)
    over_col(0, 2)
    over_row(1, 2)
    over_row(1, 3)
    over_row(1, 4)
    over_col(0, 3)
    over_col(1, 0)
    over_col(1, 1)

    for way in (0, 1):
        for r in range(TEAM - 1):
            x_copy(way, r, 0).start()
    gates()
    for s, way in steps:
        z_copy(0, s, way).wait_recv()
        x_copy(way, 0, s).start()
    over_col(1, 2)
    for r in range(1, TEAM - 1):
        order = [1] + list(range(FAR + r, 1, -1)) if r == 1 else [1, 2] + list(range(FAR + r, 2, -1))
        for s in order:
            for way in (0, 1):
                x_copy(way, r - 1, s - 1).wait_recv()
                x_copy(way, r, s).start()
        if r == 1:
            over_col(1, 3)
    if TEAM == 2:
        over_col(1, 3)
    over_col(1, 4)

    def near_blocks(half):
        last = min(4 * half + 4, FAR + 1)
        for s in range(4 * half, last):
            if s:
                for way in (0, 1):
                    z_copy(1, s, way).wait_recv()
        for way in (0, 1):
            for s in range(4 * half, last, 2):
                one = rb[way, s].astype(F32)
                two = rb[way, s + 1].astype(F32) if s + 1 < last else one
                for ph in (0, 1):
                    cut = slice(WIDE * ph, WIDE * ph + WIDE)
                    rm[way, ph, pl.ds(WIDE * s, CHUNK), :] = jnp.concatenate(
                        [one[cut], two[cut]], axis=0
                    ).astype(BF16)

    def left_lines(e):
        for q in range(ROWS):
            four = [lb[e, 4 * q + n].astype(F32) for n in range(4)]
            for ph in (0, 1):
                cut = slice(WIDE * ph, WIDE * ph + WIDE)
                lines = jnp.concatenate([f[cut] for f in four], axis=0).astype(BF16)
                for u in range(3):
                    lm[e, ph, pl.ds(128 * u + 32 * ((q + u) % 4), 32), :] = lines[
                        32 * u : 32 * u + 32
                    ]

    def c_copy(s, way):
        t = 2 * (FAR - s) + way
        return pltpu.make_async_remote_copy(
            src_ref=cs.at[t],
            dst_ref=cb.at[t],
            send_sem=csend.at[t],
            recv_sem=crecv.at[t],
            device_id={"col": col_at(-s if way == 0 else s)},
            device_id_type=MESH,
        )

    scale = (ROWS * LINES) ** -0.5
    for e in range(1, TEAM - 1):
        left_lines(e)
        own = ri[e - 1].astype(F32)
        sums = [
            nt(own[WIDE * ph : WIDE * ph + WIDE].astype(BF16), lm[e, ph]) * scale for ph in (0, 1)
        ]
        cb[2 * FAR + e] = jnp.concatenate(sums, axis=0).astype(BF16)
    near_blocks(0)
    for way in (0, 1):
        r = TEAM - 2
        for s in range(FAR + r + 1):
            x_copy(1 - way, r, s).wait_recv()
        left_lines((TEAM - 1) * way)

    for half in (0, 1):
        if half:
            near_blocks(1)
        count = min(4, FAR + 1 - 4 * half)
        for way in (0, 1):
            e = (TEAM - 1) * way
            rows = pl.ds(96 * half, WIDE * count)
            sums = [nt(rm[way, ph, rows, :], lm[e, ph]) * scale for ph in (0, 1)]
            for n in range(count):
                s = 4 * half + n
                cut = slice(WIDE * n, WIDE * n + WIDE)
                chunk = jnp.concatenate([sums[0][cut], sums[1][cut]], axis=0).astype(BF16)
                if s == 0:
                    cb[2 * FAR + e] = chunk
                else:
                    cs[2 * (FAR - s) + way] = chunk
        for n in range(count):
            s = 4 * half + n
            for way in (0, 1):
                if s:
                    c_copy(s, way).start()

    def e_copy(sub, o):
        t0, t1 = ESUBS[sub]
        dest = row_at(o)
        return pltpu.make_async_remote_copy(
            src_ref=es.at[dest, pl.ds(t0, t1 - t0)],
            dst_ref=ds.at[y, pl.ds(t0, t1 - t0)],
            send_sem=esend.at[sub, o - 1],
            recv_sem=erecv.at[sub, o - 1],
            device_id={"row": dest},
            device_id_type=MESH,
        )

    strip = lane // 32

    for sub, (t0, t1) in enumerate(ESUBS):
        for t in range(t0, t1 if t0 < 2 * FAR else t0):
            c_copy(FAR - t // 2, t % 2).wait_recv()

        @pl.loop(t0, t1)
        def _(t):
            a, b, c = (cb[t, :, pl.ds(128 * u, 128)].astype(F32) for u in range(3))

            def quarter(q):
                return jnp.where(
                    strip == q, a, jnp.where(strip == lax.rem(q + 1, 4), b, c)
                ).astype(BF16)

            for q in range(ROWS):
                es[q, t] = quarter(q)
            ds[y, t] = quarter(y)

        for o in range(1, ROWS):
            e_copy(sub, o).start()

    mixed = facl
    total = jnp.zeros((WIDE, CH), F32)
    for sub, (t0, t1) in enumerate(ESUBS):
        for o in range(1, ROWS):
            e_copy(sub, o).wait_recv()

        def add(t, total, t0=t0):
            team = team_of(t, t0 >= 2 * FAR)
            for q in range(ROWS):
                block = ds[q, t].astype(F32)
                first = pl.multiple_of((32 * q + 2 * team) * WIDE, 16)
                mixed[pl.ds(first, CHUNK), :] = block
                total = total + block[:WIDE] + block[WIDE:]
            return total

        total = lax.fori_loop(t0, t1, add, total)
    mean = total * (1.0 / CH)

    def spread(n, total):
        for m in range(8):
            off = mixed[pl.ds(pl.multiple_of((8 * n + m) * WIDE, 8), WIDE), :] - mean
            total = total + off * off
        return total

    var = lax.fori_loop(0, CH // 8, spread, jnp.zeros((WIDE, CH), F32)) * (1.0 / CH)
    stat[0] = mean
    stat[1] = lax.rsqrt(var + 1e-05)

    out = facr

    @pl.loop(0, WIDE // 4)
    def _(n):
        scaled = []
        for j in range(4):
            block = mixed[pl.ds(4 * n + j, CH, stride=WIDE), :]
            block = (block - stat[0, pl.ds(4 * n + j, 1), :]) * stat[1, pl.ds(4 * n + j, 1), :] * gb[...]
            scaled.append(block.astype(BF16).T)
        change = jnp.dot(jnp.concatenate(scaled, axis=0), wraw[4], preferred_element_type=F32)
        for j in range(4):
            for b in range(4):
                u = lax.rem(b - y + 4, 4)
                out[pl.ds(u * (32 * WIDE) + 4 * n + j, 32, stride=WIDE), :] = change[
                    CH * j + 32 * b : CH * j + 32 * b + 32
                ]

    @pl.loop(0, 6)
    def _(n):
        rows = pl.ds(pl.multiple_of(n * 384, 384), 384)
        o_ref[rows, :] = (out[rows, :] * gt[rows, :]).astype(BF16)

    for arr in (0, 1):
        for sub in range(len(YSUBS[arr])):
            for o in range(1, ROWS):
                y_copy(arr, sub, o).wait_send()
        for s, way in steps:
            z_copy(arr, s, way).wait_send()
    for way in (0, 1):
        for r in range(TEAM - 1):
            for s in range(FAR + r + 1):
                x_copy(way, r, s).wait_send()
    for s, way in steps:
        c_copy(s, way).wait_send()
    for sub in range(len(ESUBS)):
        for o in range(1, ROWS):
            e_copy(sub, o).wait_send()


def per_device(
    pair_rows, left_weight, right_weight, left_gate, right_gate, mid_gain, out_weight, out_gate
):
    pixels = pair_rows.shape[0] * pair_rows.shape[1]
    dma = pltpu.SemaphoreType.DMA
    out = pl.pallas_call(
        kernel,
        out_shape=jax.ShapeDtypeStruct((pixels, CH), BF16),
        in_specs=[pl.BlockSpec(memory_space=pltpu.HBM)] * 8,
        out_specs=pl.BlockSpec(memory_space=pltpu.VMEM),
        scratch_shapes=[
            pltpu.VMEM((pixels, CH), BF16),
            pltpu.VMEM((6, CH, CH), BF16),
            pltpu.VMEM((1, CH), F32),
            pltpu.VMEM((128 * WIDE, CH), F32),
            pltpu.VMEM((128 * WIDE, CH), BF16),
            pltpu.VMEM((2 * CH, CH), F32),
            pltpu.VMEM((4 * CH, CH), BF16),
            pltpu.VMEM((CH, CH), F32),
            pltpu.VMEM((CH * WIDE, CH), F32),
            pltpu.VMEM((CH * WIDE, CH), F32),
            pltpu.VMEM((16 * WIDE, CH), F32),
            pltpu.VMEM((2, ROWS, COLS, CHUNK, CH), BF16),
            pltpu.VMEM((2, ROWS, COLS, CHUNK, CH), BF16),
            pltpu.VMEM((2, 2 * FAR, CHUNK, 384), BF16),
            pltpu.VMEM((TEAM, COLS, CHUNK, 384), BF16),
            pltpu.VMEM((2, FAR + 1, CHUNK, 384), BF16),
            pltpu.VMEM((2, CHUNK, 384), BF16),
            pltpu.VMEM((TEAM, 2, 384, 384), BF16),
            pltpu.VMEM((2, 2, 192, 384), BF16),
            pltpu.VMEM((2 * FAR, CHUNK, 384), BF16),
            pltpu.VMEM((COLS, CHUNK, 384), BF16),
            pltpu.VMEM((ROWS, COLS, CHUNK, CH), BF16),
            pltpu.VMEM((ROWS, COLS, CHUNK, CH), BF16),
            pltpu.VMEM((pixels, CH), F32),
            pltpu.VMEM((2, WIDE, CH), F32),
            dma((10,)),
            dma((2, 5, 3)), dma((2, 5, 3)),
            dma((2, 2 * FAR)), dma((2, 2 * FAR)),
            dma((2, TEAM - 1, COLS)), dma((2, TEAM - 1, COLS)),
            dma((2 * FAR,)), dma((2 * FAR,)),
            dma((len(ESUBS), 3)), dma((len(ESUBS), 3)),
        ],
        compiler_params=pltpu.CompilerParams(
            collective_id=0, has_side_effects=True, vmem_limit_bytes=48 * 1024 * 1024
        ),
    )(
        *[
            pltpu.with_memory_space_constraint(v, pltpu.HBM)
            for v in (
                pair_rows.reshape(pixels, CH),
                left_weight, left_gate, right_weight, right_gate,
                mid_gain.reshape(1, CH), out_weight, out_gate,
            )
        ]
    )
    return out.reshape(pair_rows.shape)


def solution(mesh):
    placed = (
        P(("trial", "row"), "col", None),
        P("trial", None),
        P("trial", None),
        P("trial", None),
        P("trial", None),
        P(),
        P("trial", None),
        P("trial", None),
    )
    return jax.shard_map(
        per_device,
        mesh=mesh,
        in_specs=placed,
        out_specs=P(("trial", "row"), "col", None),
        check_vma=False,
    )
```

```python
import functools

import jax
import jax.numpy as jnp
from jax import lax
from jax.experimental import pallas as pl
from jax.experimental.pallas import tpu as pltpu
from jax.sharding import PartitionSpec as P

MESH = pl.DeviceIdType.MESH
F32, BF16 = jnp.float32, jnp.bfloat16
ROWS, COLS = 4, 16
LINES, WIDE, CH = 96, 24, 128
TEAM = 4
FAR = (COLS - TEAM) // 2
CHUNK = 2 * WIDE
YSUBS = (((0, 2), (2, 6), (6, 12), (12, 16)), ((12, 16), (10, 12), (0, 2), (2, 4), (4, 10)))
ESUBS = ((12, 16), (10, 12), (0, 2), (2, 4), (4, 6), (6, 8), (8, 10))
HALVES = ((0, 1, 6, 5), (4, 3, 2))


def sigmoid(x):
    return 0.5 + 0.5 * jnp.tanh(0.5 * x)


def nt(a, b):
    return lax.dot_general(a, b, (((1,), (1,)), ((), ())), preferred_element_type=F32)


def kernel(
    x_hbm, lw_hbm, lg_hbm, rw_hbm, rg_hbm, gain_hbm, ow_hbm, og_hbm,
    o_ref,
    x_ref, wraw, gain_ref, xf, xr, wf, wt, gb, facl, facr, fac0, zs, yb, zb, lb, rb, ri, lm, rm,
    cs, cb, es, ds, gt, stat,
    insem, sent, yrecv, zrecv, xrecv, crecv, erecv,
):
    y = lax.axis_index("row")
    z = lax.axis_index("col")

    def row_at(o):
        return lax.rem(y + o, ROWS)

    def col_at(s):
        return lax.rem(z + s + COLS, COLS)

    steps = [(s, way) for s in range(FAR, 0, -1) for way in (0, 1)]

    mats = (lw_hbm, lg_hbm, rw_hbm, rg_hbm, ow_hbm, og_hbm)
    loads = [pltpu.make_async_copy(m, wraw.at[n], insem.at[0]) for n, m in enumerate(mats)]
    loads += [pltpu.make_async_copy(gain_hbm, gain_ref, insem.at[1])]
    loads += [pltpu.make_async_copy(x_hbm, x_ref, insem.at[2])]
    for load in loads:
        load.start()

    def arrived(ref, sem):
        pltpu.make_async_remote_copy(
            src_ref=ref, dst_ref=ref, send_sem=sem, recv_sem=sem,
            device_id={"col": col_at(1)}, device_id_type=MESH,
        ).wait_recv()

    def departed(ref, sem):
        pltpu.make_async_remote_copy(
            src_ref=ref, dst_ref=ref, send_sem=sem, recv_sem=sem,
            device_id={"col": col_at(1)}, device_id_type=MESH,
        ).wait_send()

    barrier = pltpu.get_barrier_semaphore()
    for o in range(1, ROWS):
        pl.semaphore_signal(barrier, inc=1, device_id={"row": row_at(o)}, device_id_type=MESH)
    for s, way in steps:
        pl.semaphore_signal(
            barrier, inc=1, device_id={"col": col_at(s if way == 0 else -s)}, device_id_type=MESH
        )

    def team_of(t, own):
        if own:
            return lax.rem(z + COLS - (t - 2 * FAR), COLS)
        s = FAR - t // 2
        way = t % 2
        return lax.rem(z + COLS + (1 - 2 * way) * s - (TEAM - 1) * way, COLS)

    facs = (facl, facr)

    xf[pl.ds(LINES * WIDE, 32 * WIDE), :] = jnp.zeros((32 * WIDE, CH), F32)
    pltpu.make_async_copy(wraw, wraw, insem.at[0]).wait()
    loads[6].wait()
    for n in range(4):
        turned = wraw[n].astype(F32).T
        if n < 2:
            wf[pl.ds(CH * n, CH), :] = turned
        wt[pl.ds(CH * n, CH), :] = turned.astype(BF16)
    gb[...] = jnp.broadcast_to(gain_ref[...], (CH, CH)).T
    picks = []
    for n in range(2):
        for t in range(2):
            for ph in range(2):
                picks.append(wf[pl.ds(CH * n + 2 * team_of(t, False) + ph, ROWS, stride=32), :])
    first_w = jnp.concatenate(picks, axis=0).astype(BF16)
    loads[7].wait()
    xf[pl.ds(0, LINES * WIDE), :] = x_ref[...].astype(F32)

    @pl.loop(0, WIDE // 2, unroll=3)
    def _(n):
        parts = []
        for i in (2 * n, 2 * n + 1):
            for b in range(4):
                block = lax.rem(b + y, 4)
                parts.append(xf[pl.ds(block * (32 * WIDE) + i, 32, stride=WIDE), :])
        xi = jnp.concatenate(parts, axis=0).astype(BF16)
        xr[pl.ds(pl.multiple_of(2 * CH * n, 2 * CH), 2 * CH), :] = xi
        both = nt(first_w, xi)
        value = both[:16] * sigmoid(both[16:])
        for m in range(2):
            fac0[pl.ds(2 * n + m, 16, stride=WIDE), :] = value[:, CH * m : CH * m + CH]

    def project(arr):
        @pl.loop(0, WIDE // 2, unroll=3)
        def _(n):
            xi = xr[pl.ds(pl.multiple_of(2 * CH * n, 2 * CH), 2 * CH), :]
            both = nt(wt[pl.ds(2 * CH * arr, 2 * CH), :], xi)
            value = both[:CH] * sigmoid(both[CH:])
            for m in range(2):
                facs[arr][pl.ds(2 * n + m, CH, stride=WIDE), :] = value[:, CH * m : CH * m + CH]

    def y_copy(arr, sub, o):
        t0, t1 = YSUBS[arr][sub]
        dest = row_at(o)
        return pltpu.make_async_remote_copy(
            src_ref=zs.at[arr, dest, pl.ds(t0, t1 - t0)],
            dst_ref=yb.at[arr, y, pl.ds(t0, t1 - t0)],
            send_sem=sent.at[0],
            recv_sem=yrecv.at[4 * arr + sub],
            device_id={"row": dest},
            device_id_type=MESH,
        )

    def over_row(arr, sub):
        t0, t1 = YSUBS[arr][sub]

        @pl.loop(t0, t1)
        def _(t):
            team = team_of(t, t0 >= 2 * FAR)
            for q in range(ROWS):
                first = pl.multiple_of((32 * q + 2 * team) * WIDE, 16)
                zs[arr, q, t] = facs[arr][pl.ds(first, CHUNK), :].astype(BF16)
            first = pl.multiple_of((32 * y + 2 * team) * WIDE, 16)
            yb[arr, y, t] = facs[arr][pl.ds(first, CHUNK), :].astype(BF16)

        for o in range(1, ROWS):
            y_copy(arr, sub, o).start()

    def z_copy(arr, s, way):
        t = 2 * (FAR - s) + way
        dst = lb.at[(TEAM - 1) * way, z] if arr == 0 else rb.at[way, s]
        return pltpu.make_async_remote_copy(
            src_ref=zb.at[arr, t],
            dst_ref=dst,
            send_sem=sent.at[1],
            recv_sem=zrecv.at[(s - 1) // 2 if arr == 0 else 3 if s in HALVES[0] else 4],
            device_id={"col": col_at(s if way == 0 else -s)},
            device_id_type=MESH,
        )

    lane = lax.broadcasted_iota(jnp.int32, (CHUNK, CH), 1)

    def join(arr, t):
        a, b, c, d = (yb[arr, q, t].astype(F32) for q in range(ROWS))
        return jnp.concatenate(
            [
                jnp.where(lane < 96, a, b),
                jnp.where(lane < 64, b, c),
                jnp.where(lane < 32, c, d),
            ],
            axis=1,
        ).astype(BF16)

    def over_col(arr, sub):
        t0, t1 = YSUBS[arr][sub]
        arrived(yb.at[arr, pl.ds(0, 3), pl.ds(t0, t1 - t0)], yrecv.at[4 * arr + sub])
        if t0 >= 2 * FAR:
            for e in range(TEAM):
                if arr == 0:
                    lb[e, z] = join(arr, t0 + e)
                elif e in (0, TEAM - 1):
                    rb[e // (TEAM - 1), 0] = join(arr, t0 + e)
                else:
                    ri[e - 1] = join(arr, t0 + e)
            return

        @pl.loop(t0, t1)
        def _(t):
            zb[arr, t] = join(arr, t)

        for t in range(t0, t1):
            z_copy(arr, FAR - t // 2, t % 2).start()

    def x_copy(way, r, s):
        src = col_at(-s if way == 0 else s)
        e = r if way == 0 else TEAM - 1 - r
        return pltpu.make_async_remote_copy(
            src_ref=lb.at[e, src],
            dst_ref=lb.at[e + 1 - 2 * way, src],
            send_sem=sent.at[2],
            recv_sem=xrecv.at[((s + 1) // 2, 4 + s // 2, 8)[r]],
            device_id={"col": col_at(1 if way == 0 else -1)},
            device_id_type=MESH,
        )

    def gates():
        @pl.loop(0, 6)
        def _(n):
            rows = pl.ds(pl.multiple_of(n * 384, 384), 384)
            g = jnp.dot(x_ref[rows, :], wraw[5], preferred_element_type=F32)
            gt[rows, :] = sigmoid(g)

    for t in range(2):
        for q in range(ROWS):
            rows = [((2 * t + ph) * ROWS + q) * WIDE for ph in range(2)]
            zs[0, q, t] = jnp.concatenate(
                [fac0[pl.ds(first, WIDE), :] for first in rows], axis=0
            ).astype(BF16)
        rows = [pl.multiple_of(((2 * t + ph) * ROWS + y) * WIDE, 8) for ph in range(2)]
        yb[0, y, t] = jnp.concatenate(
            [fac0[pl.ds(first, WIDE), :] for first in rows], axis=0
        ).astype(BF16)
    pl.semaphore_wait(barrier, ROWS - 1 + len(steps))
    for o in range(1, ROWS):
        y_copy(0, 0, o).start()

    project(0)
    over_row(0, 1)
    over_row(0, 2)
    over_col(0, 0)
    over_row(0, 3)
    project(1)
    over_col(0, 1)
    over_row(1, 0)
    over_row(1, 1)
    over_col(0, 2)
    over_row(1, 2)
    over_row(1, 3)
    over_row(1, 4)
    over_col(0, 3)
    over_col(1, 0)
    over_col(1, 1)

    over_col(1, 2)

    for way in (0, 1):
        for r in range(TEAM - 1):
            x_copy(way, r, 0).start()
    gates()
    pairs = ((6, 5), (4, 3), (2, 1))
    for pair in pairs:
        arrived(zb.at[0, pl.ds(0, 4)], zrecv.at[(pair[1] - 1) // 2])
        for s in pair:
            for way in (0, 1):
                x_copy(way, 0, s).start()
    over_col(1, 3)
    arrived(zb.at[0, pl.ds(0, 2)], xrecv.at[0])
    for way in (0, 1):
        x_copy(way, 1, 1).start()
    for pair in pairs:
        arrived(zb.at[0, pl.ds(0, 4)], xrecv.at[(pair[1] + 1) // 2])
        for s in pair:
            for way in (0, 1):
                x_copy(way, 1, s + 1).start()
    for pair in ((1, 0), (7, 6), (5, 4), (3, 2)):
        arrived(zb.at[0, pl.ds(0, 4)], xrecv.at[4 + pair[1] // 2])
        for s in pair:
            for way in (0, 1):
                x_copy(way, 2, s + 1).start()
    over_col(1, 4)

    def near_blocks(half):
        arrived(zb.at[0, pl.ds(0, 6)], zrecv.at[3 + half])
        for way in (0, 1):
            for n in range(0, len(HALVES[half]), 2):
                one = rb[way, HALVES[half][n]].astype(F32)
                two = rb[way, HALVES[half][min(n + 1, len(HALVES[half]) - 1)]].astype(F32)
                for ph in (0, 1):
                    cut = slice(WIDE * ph, WIDE * ph + WIDE)
                    rm[way, ph, pl.ds(96 * half + WIDE * n, CHUNK), :] = jnp.concatenate(
                        [one[cut], two[cut]], axis=0
                    ).astype(BF16)

    def left_lines(e):
        for q in range(ROWS):
            four = [lb[e, 4 * q + n].astype(F32) for n in range(4)]
            for ph in (0, 1):
                cut = slice(WIDE * ph, WIDE * ph + WIDE)
                lines = jnp.concatenate([f[cut] for f in four], axis=0).astype(BF16)
                for u in range(3):
                    lm[e, ph, pl.ds(128 * u + 32 * ((q + u) % 4), 32), :] = lines[
                        32 * u : 32 * u + 32
                    ]

    def c_copy(s, way):
        t = 2 * (FAR - s) + way
        return pltpu.make_async_remote_copy(
            src_ref=cs.at[t],
            dst_ref=cb.at[t],
            send_sem=sent.at[3],
            recv_sem=crecv.at[s - 1],
            device_id={"col": col_at(-s if way == 0 else s)},
            device_id_type=MESH,
        )

    scale = (ROWS * LINES) ** -0.5
    for e in range(1, TEAM - 1):
        left_lines(e)
        own = ri[e - 1].astype(F32)
        sums = [
            nt(own[WIDE * ph : WIDE * ph + WIDE].astype(BF16), lm[e, ph]) * scale for ph in (0, 1)
        ]
        cb[2 * FAR + e] = jnp.concatenate(sums, axis=0).astype(BF16)
    near_blocks(0)
    arrived(zb.at[:, pl.ds(0, 9)], xrecv.at[8])
    for way in (0, 1):
        left_lines((TEAM - 1) * way)

    for half in (0, 1):
        if half:
            near_blocks(1)
        count = len(HALVES[half])
        for way in (0, 1):
            e = (TEAM - 1) * way
            rows = pl.ds(96 * half, WIDE * count)
            sums = [nt(rm[way, ph, rows, :], lm[e, ph]) * scale for ph in (0, 1)]
            for n, s in enumerate(HALVES[half]):
                cut = slice(WIDE * n, WIDE * n + WIDE)
                chunk = jnp.concatenate([sums[0][cut], sums[1][cut]], axis=0).astype(BF16)
                if s == 0:
                    cb[2 * FAR + e] = chunk
                else:
                    cs[2 * (FAR - s) + way] = chunk
        for s in HALVES[half]:
            for way in (0, 1):
                if s:
                    c_copy(s, way).start()

    def e_copy(sub, o):
        t0, t1 = ESUBS[sub]
        dest = row_at(o)
        return pltpu.make_async_remote_copy(
            src_ref=es.at[dest, pl.ds(t0, t1 - t0)],
            dst_ref=ds.at[y, pl.ds(t0, t1 - t0)],
            send_sem=sent.at[4],
            recv_sem=erecv.at[sub],
            device_id={"row": dest},
            device_id_type=MESH,
        )

    strip = lane // 32

    for sub, (t0, t1) in enumerate(ESUBS):
        if t0 < 2 * FAR:
            arrived(zb.at[0, pl.ds(0, 2)], crecv.at[FAR - t0 // 2 - 1])

        @pl.loop(t0, t1)
        def _(t):
            a, b, c = (cb[t, :, pl.ds(128 * u, 128)].astype(F32) for u in range(3))

            def quarter(q):
                return jnp.where(
                    strip == q, a, jnp.where(strip == lax.rem(q + 1, 4), b, c)
                ).astype(BF16)

            for q in range(ROWS):
                es[q, t] = quarter(q)
            ds[y, t] = quarter(y)

        for o in range(1, ROWS):
            e_copy(sub, o).start()

    mixed = facl
    total = jnp.zeros((WIDE, CH), F32)
    for sub, (t0, t1) in enumerate(ESUBS):
        arrived(ds.at[pl.ds(0, 3), pl.ds(t0, t1 - t0)], erecv.at[sub])

        def add(t, total, t0=t0):
            team = team_of(t, t0 >= 2 * FAR)
            for q in range(ROWS):
                block = ds[q, t].astype(F32)
                first = pl.multiple_of((32 * q + 2 * team) * WIDE, 16)
                mixed[pl.ds(first, CHUNK), :] = block
                total = total + block[:WIDE] + block[WIDE:]
            return total

        total = lax.fori_loop(t0, t1, add, total)
    mean = total * (1.0 / CH)

    def spread(n, total):
        for m in range(8):
            off = mixed[pl.ds(pl.multiple_of((8 * n + m) * WIDE, 8), WIDE), :] - mean
            total = total + off * off
        return total

    var = lax.fori_loop(0, CH // 8, spread, jnp.zeros((WIDE, CH), F32)) * (1.0 / CH)
    stat[0] = mean
    stat[1] = lax.rsqrt(var + 1e-05)

    out = facr

    @pl.loop(0, WIDE // 4)
    def _(n):
        scaled = []
        for j in range(4):
            block = mixed[pl.ds(4 * n + j, CH, stride=WIDE), :]
            block = (block - stat[0, pl.ds(4 * n + j, 1), :]) * stat[1, pl.ds(4 * n + j, 1), :] * gb[...]
            scaled.append(block.astype(BF16).T)
        change = jnp.dot(jnp.concatenate(scaled, axis=0), wraw[4], preferred_element_type=F32)
        for j in range(4):
            for b in range(4):
                u = lax.rem(b - y + 4, 4)
                out[pl.ds(u * (32 * WIDE) + 4 * n + j, 32, stride=WIDE), :] = change[
                    CH * j + 32 * b : CH * j + 32 * b + 32
                ]

    @pl.loop(0, 6)
    def _(n):
        rows = pl.ds(pl.multiple_of(n * 384, 384), 384)
        o_ref[rows, :] = (out[rows, :] * gt[rows, :]).astype(BF16)

    departed(zs.at[:, pl.ds(0, 3)], sent.at[0])
    departed(zb, sent.at[1])
    departed(lb.at[pl.ds(0, 3)], sent.at[2])
    departed(cs, sent.at[3])
    departed(es.at[pl.ds(0, 3)], sent.at[4])


def per_device(
    pair_rows, left_weight, right_weight, left_gate, right_gate, mid_gain, out_weight, out_gate
):
    pixels = pair_rows.shape[0] * pair_rows.shape[1]
    dma = pltpu.SemaphoreType.DMA
    out = pl.pallas_call(
        kernel,
        out_shape=jax.ShapeDtypeStruct((pixels, CH), BF16),
        in_specs=[pl.BlockSpec(memory_space=pltpu.HBM)] * 8,
        out_specs=pl.BlockSpec(memory_space=pltpu.VMEM),
        scratch_shapes=[
            pltpu.VMEM((pixels, CH), BF16),
            pltpu.VMEM((6, CH, CH), BF16),
            pltpu.VMEM((1, CH), F32),
            pltpu.VMEM((128 * WIDE, CH), F32),
            pltpu.VMEM((128 * WIDE, CH), BF16),
            pltpu.VMEM((2 * CH, CH), F32),
            pltpu.VMEM((4 * CH, CH), BF16),
            pltpu.VMEM((CH, CH), F32),
            pltpu.VMEM((CH * WIDE, CH), F32),
            pltpu.VMEM((CH * WIDE, CH), F32),
            pltpu.VMEM((16 * WIDE, CH), F32),
            pltpu.VMEM((2, ROWS, COLS, CHUNK, CH), BF16),
            pltpu.VMEM((2, ROWS, COLS, CHUNK, CH), BF16),
            pltpu.VMEM((2, 2 * FAR, CHUNK, 384), BF16),
            pltpu.VMEM((TEAM, COLS, CHUNK, 384), BF16),
            pltpu.VMEM((2, FAR + 1, CHUNK, 384), BF16),
            pltpu.VMEM((2, CHUNK, 384), BF16),
            pltpu.VMEM((TEAM, 2, 384, 384), BF16),
            pltpu.VMEM((2, 2, 192, 384), BF16),
            pltpu.VMEM((2 * FAR, CHUNK, 384), BF16),
            pltpu.VMEM((COLS, CHUNK, 384), BF16),
            pltpu.VMEM((ROWS, COLS, CHUNK, CH), BF16),
            pltpu.VMEM((ROWS, COLS, CHUNK, CH), BF16),
            pltpu.VMEM((pixels, CH), F32),
            pltpu.VMEM((2, WIDE, CH), F32),
            dma((3,)), dma((5,)), dma((9,)), dma((5,)), dma((9,)), dma((FAR,)), dma((len(ESUBS),)),
        ],
        compiler_params=pltpu.CompilerParams(
            collective_id=0, has_side_effects=True, vmem_limit_bytes=48 * 1024 * 1024
        ),
    )(
        *[
            pltpu.with_memory_space_constraint(v, pltpu.HBM)
            for v in (
                pair_rows.reshape(pixels, CH),
                left_weight, left_gate, right_weight, right_gate,
                mid_gain.reshape(1, CH), out_weight, out_gate,
            )
        ]
    )
    return out.reshape(pair_rows.shape)


def solution(mesh):
    placed = (
        P(("trial", "row"), "col", None),
        P("trial", None),
        P("trial", None),
        P("trial", None),
        P("trial", None),
        P(),
        P("trial", None),
        P("trial", None),
    )
    return jax.shard_map(
        per_device,
        mesh=mesh,
        in_specs=placed,
        out_specs=P(("trial", "row"), "col", None),
        check_vma=False,
    )
```

```python
import functools

import jax
import jax.numpy as jnp
from jax import lax
from jax.experimental import pallas as pl
from jax.experimental.pallas import tpu as pltpu
from jax.sharding import PartitionSpec as P

MESH = pl.DeviceIdType.MESH
F32, BF16 = jnp.float32, jnp.bfloat16
ROWS, COLS = 4, 16
LINES, WIDE, CH = 96, 24, 128
TEAM = 6
FAR = (COLS - TEAM) // 2
CHUNK = 2 * WIDE
YSUBS = (((0, 2), (2, 6), (6, 10), (10, 16)), ((10, 16), (8, 10), (0, 2), (2, 4), (4, 8)))
ESUBS = ((10, 16), (8, 10), (0, 2), (2, 4), (4, 6), (6, 8))
HALVES = ((0, 1, 5, 4), (3, 2))
DIRECT = ((5,), (4, 3), (2, 1))
ORDERS = [[0, 5, 4, 3, 2, 1]]
while len(ORDERS) < TEAM - 1:
    ORDERS.append([0] + [s + 1 for s in ORDERS[-1]])
GROUPS = [[order[n : n + 2] for n in range(0, len(order), 2)] for order in ORDERS]
GROUPS[-1] = [ORDERS[-1]]
XBASE = [sum(len(g) for g in GROUPS[:r]) for r in range(TEAM)]


def hand_sem(r, s):
    return XBASE[r] + [s in group for group in GROUPS[r]].index(True)


def sigmoid(x):
    return 0.5 + 0.5 * jnp.tanh(0.5 * x)


def nt(a, b):
    return lax.dot_general(a, b, (((1,), (1,)), ((), ())), preferred_element_type=F32)


def kernel(
    x_hbm, lw_hbm, lg_hbm, rw_hbm, rg_hbm, gain_hbm, ow_hbm, og_hbm,
    o_ref,
    x_ref, wraw, gain_ref, xf, xr, wf, wt, gb, facl, facr, fac0, zs, yb, zb, lb, rb, ri, lm, rm,
    cs, cb, es, ds, gt, stat,
    insem, sent, yrecv, zrecv, xrecv, crecv, erecv,
):
    y = lax.axis_index("row")
    z = lax.axis_index("col")

    def row_at(o):
        return lax.rem(y + o, ROWS)

    def col_at(s):
        return lax.rem(z + s + COLS, COLS)

    steps = [(s, way) for s in range(FAR, 0, -1) for way in (0, 1)]

    mats = (lw_hbm, lg_hbm, rw_hbm, rg_hbm, ow_hbm, og_hbm)
    loads = [pltpu.make_async_copy(m, wraw.at[n], insem.at[0]) for n, m in enumerate(mats)]
    loads += [pltpu.make_async_copy(gain_hbm, gain_ref, insem.at[1])]
    loads += [pltpu.make_async_copy(x_hbm, x_ref, insem.at[2])]
    for load in loads:
        load.start()

    def arrived(ref, sem):
        pltpu.make_async_remote_copy(
            src_ref=ref, dst_ref=ref, send_sem=sem, recv_sem=sem,
            device_id={"col": col_at(1)}, device_id_type=MESH,
        ).wait_recv()

    def departed(ref, sem):
        pltpu.make_async_remote_copy(
            src_ref=ref, dst_ref=ref, send_sem=sem, recv_sem=sem,
            device_id={"col": col_at(1)}, device_id_type=MESH,
        ).wait_send()

    barrier = pltpu.get_barrier_semaphore()
    for o in range(1, ROWS):
        pl.semaphore_signal(barrier, inc=1, device_id={"row": row_at(o)}, device_id_type=MESH)
    for s, way in steps:
        pl.semaphore_signal(
            barrier, inc=1, device_id={"col": col_at(s if way == 0 else -s)}, device_id_type=MESH
        )

    def team_of(t, own):
        if own:
            return lax.rem(z + COLS - (t - 2 * FAR), COLS)
        s = FAR - t // 2
        way = t % 2
        return lax.rem(z + COLS + (1 - 2 * way) * s - (TEAM - 1) * way, COLS)

    facs = (facl, facr)

    xf[pl.ds(LINES * WIDE, 32 * WIDE), :] = jnp.zeros((32 * WIDE, CH), F32)
    pltpu.make_async_copy(wraw, wraw, insem.at[0]).wait()
    loads[6].wait()
    for n in range(4):
        turned = wraw[n].astype(F32).T
        if n < 2:
            wf[pl.ds(CH * n, CH), :] = turned
        wt[pl.ds(CH * n, CH), :] = turned.astype(BF16)
    gb[...] = jnp.broadcast_to(gain_ref[...], (CH, CH)).T
    picks = []
    for n in range(2):
        for t in range(2):
            for ph in range(2):
                picks.append(wf[pl.ds(CH * n + 2 * team_of(t, False) + ph, ROWS, stride=32), :])
    first_w = jnp.concatenate(picks, axis=0).astype(BF16)
    loads[7].wait()
    xf[pl.ds(0, LINES * WIDE), :] = x_ref[...].astype(F32)

    @pl.loop(0, WIDE // 2, unroll=3)
    def _(n):
        parts = []
        for i in (2 * n, 2 * n + 1):
            for b in range(4):
                block = lax.rem(b + y, 4)
                parts.append(xf[pl.ds(block * (32 * WIDE) + i, 32, stride=WIDE), :])
        xi = jnp.concatenate(parts, axis=0).astype(BF16)
        xr[pl.ds(pl.multiple_of(2 * CH * n, 2 * CH), 2 * CH), :] = xi
        both = nt(first_w, xi)
        value = both[:16] * sigmoid(both[16:])
        for m in range(2):
            fac0[pl.ds(2 * n + m, 16, stride=WIDE), :] = value[:, CH * m : CH * m + CH]

    def project(arr):
        @pl.loop(0, WIDE // 2, unroll=3)
        def _(n):
            xi = xr[pl.ds(pl.multiple_of(2 * CH * n, 2 * CH), 2 * CH), :]
            both = nt(wt[pl.ds(2 * CH * arr, 2 * CH), :], xi)
            value = both[:CH] * sigmoid(both[CH:])
            for m in range(2):
                facs[arr][pl.ds(2 * n + m, CH, stride=WIDE), :] = value[:, CH * m : CH * m + CH]

    def y_copy(arr, sub, o):
        t0, t1 = YSUBS[arr][sub]
        dest = row_at(o)
        return pltpu.make_async_remote_copy(
            src_ref=zs.at[arr, dest, pl.ds(t0, t1 - t0)],
            dst_ref=yb.at[arr, y, pl.ds(t0, t1 - t0)],
            send_sem=sent.at[0],
            recv_sem=yrecv.at[4 * arr + sub],
            device_id={"row": dest},
            device_id_type=MESH,
        )

    def over_row(arr, sub):
        t0, t1 = YSUBS[arr][sub]

        @pl.loop(t0, t1)
        def _(t):
            team = team_of(t, t0 >= 2 * FAR)
            for q in range(ROWS):
                first = pl.multiple_of((32 * q + 2 * team) * WIDE, 16)
                zs[arr, q, t] = facs[arr][pl.ds(first, CHUNK), :].astype(BF16)
            first = pl.multiple_of((32 * y + 2 * team) * WIDE, 16)
            yb[arr, y, t] = facs[arr][pl.ds(first, CHUNK), :].astype(BF16)

        for o in range(1, ROWS):
            y_copy(arr, sub, o).start()

    def z_copy(arr, s, way):
        t = 2 * (FAR - s) + way
        dst = lb.at[(TEAM - 1) * way, z] if arr == 0 else rb.at[way, s]
        return pltpu.make_async_remote_copy(
            src_ref=zb.at[arr, t],
            dst_ref=dst,
            send_sem=sent.at[1],
            recv_sem=zrecv.at[(s - 1) // 2 if arr == 0 else 3 if s in HALVES[0] else 4],
            device_id={"col": col_at(s if way == 0 else -s)},
            device_id_type=MESH,
        )

    lane = lax.broadcasted_iota(jnp.int32, (CHUNK, CH), 1)

    def join(arr, t):
        a, b, c, d = (yb[arr, q, t].astype(F32) for q in range(ROWS))
        return jnp.concatenate(
            [
                jnp.where(lane < 96, a, b),
                jnp.where(lane < 64, b, c),
                jnp.where(lane < 32, c, d),
            ],
            axis=1,
        ).astype(BF16)

    def over_col(arr, sub):
        t0, t1 = YSUBS[arr][sub]
        arrived(yb.at[arr, pl.ds(0, 3), pl.ds(t0, t1 - t0)], yrecv.at[4 * arr + sub])
        if t0 >= 2 * FAR:
            for e in range(TEAM):
                if arr == 0:
                    lb[e, z] = join(arr, t0 + e)
                elif e in (0, TEAM - 1):
                    rb[e // (TEAM - 1), 0] = join(arr, t0 + e)
                else:
                    ri[e - 1] = join(arr, t0 + e)
            return

        @pl.loop(t0, t1)
        def _(t):
            zb[arr, t] = join(arr, t)

        for t in range(t0, t1):
            z_copy(arr, FAR - t // 2, t % 2).start()

    def x_copy(way, r, s):
        src = col_at(-s if way == 0 else s)
        e = r if way == 0 else TEAM - 1 - r
        return pltpu.make_async_remote_copy(
            src_ref=lb.at[e, src],
            dst_ref=lb.at[e + 1 - 2 * way, src],
            send_sem=sent.at[2],
            recv_sem=xrecv.at[hand_sem(r, s)],
            device_id={"col": col_at(1 if way == 0 else -1)},
            device_id_type=MESH,
        )

    def gates():
        @pl.loop(0, 6)
        def _(n):
            rows = pl.ds(pl.multiple_of(n * 384, 384), 384)
            g = jnp.dot(x_ref[rows, :], wraw[5], preferred_element_type=F32)
            gt[rows, :] = sigmoid(g)

    for t in range(2):
        for q in range(ROWS):
            rows = [((2 * t + ph) * ROWS + q) * WIDE for ph in range(2)]
            zs[0, q, t] = jnp.concatenate(
                [fac0[pl.ds(first, WIDE), :] for first in rows], axis=0
            ).astype(BF16)
        rows = [pl.multiple_of(((2 * t + ph) * ROWS + y) * WIDE, 8) for ph in range(2)]
        yb[0, y, t] = jnp.concatenate(
            [fac0[pl.ds(first, WIDE), :] for first in rows], axis=0
        ).astype(BF16)
    pl.semaphore_wait(barrier, ROWS - 1 + len(steps))
    for o in range(1, ROWS):
        y_copy(0, 0, o).start()

    project(0)
    over_row(0, 1)
    over_row(0, 2)
    over_col(0, 0)
    over_row(0, 3)
    project(1)
    over_col(0, 1)
    over_row(1, 0)
    over_row(1, 1)
    over_col(0, 2)
    over_row(1, 2)
    over_row(1, 3)
    over_row(1, 4)
    over_col(0, 3)
    over_col(1, 0)
    over_col(1, 1)

    over_col(1, 2)

    for way in (0, 1):
        for r in range(TEAM - 1):
            x_copy(way, r, 0).start()
    gates()
    for near in DIRECT:
        arrived(zb.at[0, pl.ds(0, 2 * len(near))], zrecv.at[(near[-1] - 1) // 2])
        for s in near:
            for way in (0, 1):
                x_copy(way, 0, s).start()
    over_col(1, 3)
    for r in range(1, TEAM - 1):
        for n, group in enumerate(GROUPS[r - 1]):
            arrived(zb.at[0, pl.ds(0, 2 * len(group))], xrecv.at[XBASE[r - 1] + n])
            for s in group:
                for way in (0, 1):
                    x_copy(way, r, s + 1).start()
    over_col(1, 4)

    def near_blocks(half):
        arrived(zb.at[0, pl.ds(0, 2 * sum(s > 0 for s in HALVES[half]))], zrecv.at[3 + half])
        for way in (0, 1):
            for n in range(0, len(HALVES[half]), 2):
                one = rb[way, HALVES[half][n]].astype(F32)
                two = rb[way, HALVES[half][min(n + 1, len(HALVES[half]) - 1)]].astype(F32)
                for ph in (0, 1):
                    cut = slice(WIDE * ph, WIDE * ph + WIDE)
                    rm[way, ph, pl.ds(96 * half + WIDE * n, CHUNK), :] = jnp.concatenate(
                        [one[cut], two[cut]], axis=0
                    ).astype(BF16)

    def left_lines(e):
        for q in range(ROWS):
            four = [lb[e, 4 * q + n].astype(F32) for n in range(4)]
            for ph in (0, 1):
                cut = slice(WIDE * ph, WIDE * ph + WIDE)
                lines = jnp.concatenate([f[cut] for f in four], axis=0).astype(BF16)
                for u in range(3):
                    lm[e, ph, pl.ds(128 * u + 32 * ((q + u) % 4), 32), :] = lines[
                        32 * u : 32 * u + 32
                    ]

    def c_copy(s, way):
        t = 2 * (FAR - s) + way
        return pltpu.make_async_remote_copy(
            src_ref=cs.at[t],
            dst_ref=cb.at[t],
            send_sem=sent.at[3],
            recv_sem=crecv.at[s - 1],
            device_id={"col": col_at(-s if way == 0 else s)},
            device_id_type=MESH,
        )

    scale = (ROWS * LINES) ** -0.5
    for e in range(1, TEAM - 1):
        left_lines(e)
        own = ri[e - 1].astype(F32)
        sums = [
            nt(own[WIDE * ph : WIDE * ph + WIDE].astype(BF16), lm[e, ph]) * scale for ph in (0, 1)
        ]
        cb[2 * FAR + e] = jnp.concatenate(sums, axis=0).astype(BF16)
    near_blocks(0)
    arrived(zb, xrecv.at[XBASE[TEAM - 2]])
    for way in (0, 1):
        left_lines((TEAM - 1) * way)

    for half in (0, 1):
        if half:
            near_blocks(1)
        count = len(HALVES[half])
        for way in (0, 1):
            e = (TEAM - 1) * way
            rows = pl.ds(96 * half, WIDE * count)
            sums = [nt(rm[way, ph, rows, :], lm[e, ph]) * scale for ph in (0, 1)]
            for n, s in enumerate(HALVES[half]):
                cut = slice(WIDE * n, WIDE * n + WIDE)
                chunk = jnp.concatenate([sums[0][cut], sums[1][cut]], axis=0).astype(BF16)
                if s == 0:
                    cb[2 * FAR + e] = chunk
                else:
                    cs[2 * (FAR - s) + way] = chunk
        for s in HALVES[half]:
            for way in (0, 1):
                if s:
                    c_copy(s, way).start()

    def e_copy(sub, o):
        t0, t1 = ESUBS[sub]
        dest = row_at(o)
        return pltpu.make_async_remote_copy(
            src_ref=es.at[dest, pl.ds(t0, t1 - t0)],
            dst_ref=ds.at[y, pl.ds(t0, t1 - t0)],
            send_sem=sent.at[4],
            recv_sem=erecv.at[sub],
            device_id={"row": dest},
            device_id_type=MESH,
        )

    strip = lane // 32

    for sub, (t0, t1) in enumerate(ESUBS):
        if t0 < 2 * FAR:
            arrived(zb.at[0, pl.ds(0, 2)], crecv.at[FAR - t0 // 2 - 1])

        @pl.loop(t0, t1)
        def _(t):
            a, b, c = (cb[t, :, pl.ds(128 * u, 128)].astype(F32) for u in range(3))

            def quarter(q):
                return jnp.where(
                    strip == q, a, jnp.where(strip == lax.rem(q + 1, 4), b, c)
                ).astype(BF16)

            for q in range(ROWS):
                es[q, t] = quarter(q)
            ds[y, t] = quarter(y)

        for o in range(1, ROWS):
            e_copy(sub, o).start()

    mixed = facl
    total = jnp.zeros((WIDE, CH), F32)
    for sub, (t0, t1) in enumerate(ESUBS):
        arrived(ds.at[pl.ds(0, 3), pl.ds(t0, t1 - t0)], erecv.at[sub])

        def add(t, total, t0=t0):
            team = team_of(t, t0 >= 2 * FAR)
            for q in range(ROWS):
                block = ds[q, t].astype(F32)
                first = pl.multiple_of((32 * q + 2 * team) * WIDE, 16)
                mixed[pl.ds(first, CHUNK), :] = block
                total = total + block[:WIDE] + block[WIDE:]
            return total

        total = lax.fori_loop(t0, t1, add, total)
    mean = total * (1.0 / CH)

    def spread(n, total):
        for m in range(8):
            off = mixed[pl.ds(pl.multiple_of((8 * n + m) * WIDE, 8), WIDE), :] - mean
            total = total + off * off
        return total

    var = lax.fori_loop(0, CH // 8, spread, jnp.zeros((WIDE, CH), F32)) * (1.0 / CH)
    stat[0] = mean
    stat[1] = lax.rsqrt(var + 1e-05)

    out = facr

    @pl.loop(0, WIDE // 4)
    def _(n):
        scaled = []
        for j in range(4):
            block = mixed[pl.ds(4 * n + j, CH, stride=WIDE), :]
            block = (block - stat[0, pl.ds(4 * n + j, 1), :]) * stat[1, pl.ds(4 * n + j, 1), :] * gb[...]
            scaled.append(block.astype(BF16).T)
        change = jnp.dot(jnp.concatenate(scaled, axis=0), wraw[4], preferred_element_type=F32)
        for j in range(4):
            for b in range(4):
                u = lax.rem(b - y + 4, 4)
                out[pl.ds(u * (32 * WIDE) + 4 * n + j, 32, stride=WIDE), :] = change[
                    CH * j + 32 * b : CH * j + 32 * b + 32
                ]

    @pl.loop(0, 6)
    def _(n):
        rows = pl.ds(pl.multiple_of(n * 384, 384), 384)
        o_ref[rows, :] = (out[rows, :] * gt[rows, :]).astype(BF16)

    departed(zs.at[:, pl.ds(0, 3)], sent.at[0])
    departed(zb, sent.at[1])
    departed(lb.at[pl.ds(0, TEAM - 1)], sent.at[2])
    departed(cs, sent.at[3])
    departed(es.at[pl.ds(0, 3)], sent.at[4])


def per_device(
    pair_rows, left_weight, right_weight, left_gate, right_gate, mid_gain, out_weight, out_gate
):
    pixels = pair_rows.shape[0] * pair_rows.shape[1]
    dma = pltpu.SemaphoreType.DMA
    out = pl.pallas_call(
        kernel,
        out_shape=jax.ShapeDtypeStruct((pixels, CH), BF16),
        in_specs=[pl.BlockSpec(memory_space=pltpu.HBM)] * 8,
        out_specs=pl.BlockSpec(memory_space=pltpu.VMEM),
        scratch_shapes=[
            pltpu.VMEM((pixels, CH), BF16),
            pltpu.VMEM((6, CH, CH), BF16),
            pltpu.VMEM((1, CH), F32),
            pltpu.VMEM((128 * WIDE, CH), F32),
            pltpu.VMEM((128 * WIDE, CH), BF16),
            pltpu.VMEM((2 * CH, CH), F32),
            pltpu.VMEM((4 * CH, CH), BF16),
            pltpu.VMEM((CH, CH), F32),
            pltpu.VMEM((CH * WIDE, CH), F32),
            pltpu.VMEM((CH * WIDE, CH), F32),
            pltpu.VMEM((16 * WIDE, CH), F32),
            pltpu.VMEM((2, ROWS, COLS, CHUNK, CH), BF16),
            pltpu.VMEM((2, ROWS, COLS, CHUNK, CH), BF16),
            pltpu.VMEM((2, 2 * FAR, CHUNK, 384), BF16),
            pltpu.VMEM((TEAM, COLS, CHUNK, 384), BF16),
            pltpu.VMEM((2, FAR + 1, CHUNK, 384), BF16),
            pltpu.VMEM((TEAM - 2, CHUNK, 384), BF16),
            pltpu.VMEM((TEAM, 2, 384, 384), BF16),
            pltpu.VMEM((2, 2, 192, 384), BF16),
            pltpu.VMEM((2 * FAR, CHUNK, 384), BF16),
            pltpu.VMEM((COLS, CHUNK, 384), BF16),
            pltpu.VMEM((ROWS, COLS, CHUNK, CH), BF16),
            pltpu.VMEM((ROWS, COLS, CHUNK, CH), BF16),
            pltpu.VMEM((pixels, CH), F32),
            pltpu.VMEM((2, WIDE, CH), F32),
            dma((3,)), dma((5,)), dma((9,)), dma((5,)), dma((XBASE[-1],)), dma((FAR,)), dma((len(ESUBS),)),
        ],
        compiler_params=pltpu.CompilerParams(
            collective_id=0, has_side_effects=True, vmem_limit_bytes=48 * 1024 * 1024
        ),
    )(
        *[
            pltpu.with_memory_space_constraint(v, pltpu.HBM)
            for v in (
                pair_rows.reshape(pixels, CH),
                left_weight, left_gate, right_weight, right_gate,
                mid_gain.reshape(1, CH), out_weight, out_gate,
            )
        ]
    )
    return out.reshape(pair_rows.shape)


def solution(mesh):
    placed = (
        P(("trial", "row"), "col", None),
        P("trial", None),
        P("trial", None),
        P("trial", None),
        P("trial", None),
        P(),
        P("trial", None),
        P("trial", None),
    )
    return jax.shard_map(
        per_device,
        mesh=mesh,
        in_specs=placed,
        out_specs=P(("trial", "row"), "col", None),
        check_vma=False,
    )
```

```python
import functools

import jax
import jax.numpy as jnp
from jax import lax
from jax.experimental import pallas as pl
from jax.experimental.pallas import tpu as pltpu
from jax.sharding import PartitionSpec as P

MESH = pl.DeviceIdType.MESH
F32, BF16 = jnp.float32, jnp.bfloat16
ROWS, COLS = 4, 16
LINES, WIDE, CH = 96, 24, 128
TEAM = 6
FAR = (COLS - TEAM) // 2
CHUNK = 2 * WIDE
YSUBS = (((0, 2), (2, 6), (6, 10), (10, 16)), ((10, 16), (0, 2), (2, 4), (4, 6), (6, 10)))
ESUBS = ((10, 16), (0, 2), (2, 4), (4, 6), (6, 8), (8, 10))
HALVES = ((0, 5, 4, 3), (2, 1))
DIRECT = ((5,), (4, 3), (2, 1))
ORDERS = [[0, 5, 4, 3, 2, 1]]
while len(ORDERS) < TEAM - 1:
    ORDERS.append([0] + [s + 1 for s in ORDERS[-1]])
GROUPS = [[order[n : n + 2] for n in range(0, len(order), 2)] for order in ORDERS]
GROUPS[-1] = [ORDERS[-1]]
XBASE = [sum(len(g) for g in GROUPS[:r]) for r in range(TEAM)]


def hand_sem(r, s):
    return XBASE[r] + [s in group for group in GROUPS[r]].index(True)


def sigmoid(x):
    return 0.5 + 0.5 * jnp.tanh(0.5 * x)


def nt(a, b):
    return lax.dot_general(a, b, (((1,), (1,)), ((), ())), preferred_element_type=F32)


def kernel(
    x_hbm, lw_hbm, lg_hbm, rw_hbm, rg_hbm, gain_hbm, ow_hbm, og_hbm,
    o_ref,
    x_ref, wraw, gain_ref, xf, xr, wf, wt, gb, facl, facr, fac0, zs, yb, zb, lb, rb, ri, lm, rm,
    cs, cb, es, ds, gt, stat,
    insem, sent, yrecv, zrecv, xrecv, crecv, erecv,
):
    y = lax.axis_index("row")
    z = lax.axis_index("col")

    def row_at(o):
        return lax.rem(y + o, ROWS)

    def col_at(s):
        return lax.rem(z + s + COLS, COLS)

    steps = [(s, way) for s in range(FAR, 0, -1) for way in (0, 1)]

    mats = (lw_hbm, lg_hbm, rw_hbm, rg_hbm, ow_hbm, og_hbm)
    loads = [pltpu.make_async_copy(m, wraw.at[n], insem.at[0]) for n, m in enumerate(mats)]
    loads += [pltpu.make_async_copy(gain_hbm, gain_ref, insem.at[1])]
    loads += [pltpu.make_async_copy(x_hbm, x_ref, insem.at[2])]
    for load in loads:
        load.start()

    def arrived(ref, sem):
        pltpu.make_async_remote_copy(
            src_ref=ref, dst_ref=ref, send_sem=sem, recv_sem=sem,
            device_id={"col": col_at(1)}, device_id_type=MESH,
        ).wait_recv()

    def departed(ref, sem):
        pltpu.make_async_remote_copy(
            src_ref=ref, dst_ref=ref, send_sem=sem, recv_sem=sem,
            device_id={"col": col_at(1)}, device_id_type=MESH,
        ).wait_send()

    barrier = pltpu.get_barrier_semaphore()
    for o in range(1, ROWS):
        pl.semaphore_signal(barrier, inc=1, device_id={"row": row_at(o)}, device_id_type=MESH)
    for s, way in steps:
        pl.semaphore_signal(
            barrier, inc=1, device_id={"col": col_at(s if way == 0 else -s)}, device_id_type=MESH
        )

    def team_of(t, own):
        if own:
            return lax.rem(z + COLS - (t - 2 * FAR), COLS)
        s = FAR - t // 2
        way = t % 2
        return lax.rem(z + COLS + (1 - 2 * way) * s - (TEAM - 1) * way, COLS)

    facs = (facl, facr)

    xf[pl.ds(LINES * WIDE, 32 * WIDE), :] = jnp.zeros((32 * WIDE, CH), F32)
    pltpu.make_async_copy(wraw, wraw, insem.at[0]).wait()
    loads[6].wait()
    for n in range(4):
        turned = wraw[n].astype(F32).T
        if n < 2:
            wf[pl.ds(CH * n, CH), :] = turned
        wt[pl.ds(CH * n, CH), :] = turned.astype(BF16)
    gb[...] = jnp.broadcast_to(gain_ref[...], (CH, CH)).T
    picks = []
    for n in range(2):
        for t in range(2):
            for ph in range(2):
                picks.append(wf[pl.ds(CH * n + 2 * team_of(t, False) + ph, ROWS, stride=32), :])
    first_w = jnp.concatenate(picks, axis=0).astype(BF16)
    loads[7].wait()
    xf[pl.ds(0, LINES * WIDE), :] = x_ref[...].astype(F32)

    @pl.loop(0, WIDE // 2, unroll=6)
    def _(n):
        parts = []
        for i in (2 * n, 2 * n + 1):
            for b in range(4):
                block = lax.rem(b + y, 4)
                parts.append(xf[pl.ds(block * (32 * WIDE) + i, 32, stride=WIDE), :])
        xi = jnp.concatenate(parts, axis=0).astype(BF16)
        xr[pl.ds(pl.multiple_of(2 * CH * n, 2 * CH), 2 * CH), :] = xi
        both = nt(first_w, xi)
        value = both[:16] * sigmoid(both[16:])
        for m in range(2):
            fac0[pl.ds(2 * n + m, 16, stride=WIDE), :] = value[:, CH * m : CH * m + CH]

    def project(arr):
        @pl.loop(0, WIDE // 2, unroll=6)
        def _(n):
            xi = xr[pl.ds(pl.multiple_of(2 * CH * n, 2 * CH), 2 * CH), :]
            both = nt(wt[pl.ds(2 * CH * arr, 2 * CH), :], xi)
            value = both[:CH] * sigmoid(both[CH:])
            for m in range(2):
                facs[arr][pl.ds(2 * n + m, CH, stride=WIDE), :] = value[:, CH * m : CH * m + CH]

    def y_copy(arr, sub, o):
        t0, t1 = YSUBS[arr][sub]
        dest = row_at(o)
        return pltpu.make_async_remote_copy(
            src_ref=zs.at[arr, dest, pl.ds(t0, t1 - t0)],
            dst_ref=yb.at[arr, y, pl.ds(t0, t1 - t0)],
            send_sem=sent.at[0],
            recv_sem=yrecv.at[4 * arr + sub],
            device_id={"row": dest},
            device_id_type=MESH,
        )

    def over_row(arr, sub):
        t0, t1 = YSUBS[arr][sub]

        @pl.loop(t0, t1)
        def _(t):
            team = team_of(t, t0 >= 2 * FAR)
            for q in range(ROWS):
                first = pl.multiple_of((32 * q + 2 * team) * WIDE, 16)
                zs[arr, q, t] = facs[arr][pl.ds(first, CHUNK), :].astype(BF16)
            first = pl.multiple_of((32 * y + 2 * team) * WIDE, 16)
            yb[arr, y, t] = facs[arr][pl.ds(first, CHUNK), :].astype(BF16)

        for o in (2, 1, 3):
            y_copy(arr, sub, o).start()

    def z_copy(arr, s, way):
        t = 2 * (FAR - s) + way
        dst = lb.at[(TEAM - 1) * way, z] if arr == 0 else rb.at[way, s]
        return pltpu.make_async_remote_copy(
            src_ref=zb.at[arr, t],
            dst_ref=dst,
            send_sem=sent.at[1],
            recv_sem=zrecv.at[(s - 1) // 2 if arr == 0 else 3 if s in HALVES[0] else 4],
            device_id={"col": col_at(s if way == 0 else -s)},
            device_id_type=MESH,
        )

    lane = lax.broadcasted_iota(jnp.int32, (CHUNK, CH), 1)

    def join(arr, t):
        a, b, c, d = (yb[arr, q, t].astype(F32) for q in range(ROWS))
        return jnp.concatenate(
            [
                jnp.where(lane < 96, a, b),
                jnp.where(lane < 64, b, c),
                jnp.where(lane < 32, c, d),
            ],
            axis=1,
        ).astype(BF16)

    def over_col(arr, sub):
        t0, t1 = YSUBS[arr][sub]
        arrived(yb.at[arr, pl.ds(0, 3), pl.ds(t0, t1 - t0)], yrecv.at[4 * arr + sub])
        if t0 >= 2 * FAR:
            for e in range(TEAM):
                if arr == 0:
                    lb[e, z] = join(arr, t0 + e)
                elif e in (0, TEAM - 1):
                    rb[e // (TEAM - 1), 0] = join(arr, t0 + e)
                else:
                    ri[e - 1] = join(arr, t0 + e)
            return

        @pl.loop(t0, t1)
        def _(t):
            zb[arr, t] = join(arr, t)

        for t in range(t0, t1):
            z_copy(arr, FAR - t // 2, t % 2).start()

    def x_copy(way, r, s):
        src = col_at(-s if way == 0 else s)
        e = r if way == 0 else TEAM - 1 - r
        return pltpu.make_async_remote_copy(
            src_ref=lb.at[e, src],
            dst_ref=lb.at[e + 1 - 2 * way, src],
            send_sem=sent.at[2],
            recv_sem=xrecv.at[hand_sem(r, s)],
            device_id={"col": col_at(1 if way == 0 else -1)},
            device_id_type=MESH,
        )

    def gates():
        @pl.loop(0, 6)
        def _(n):
            rows = pl.ds(pl.multiple_of(n * 384, 384), 384)
            g = jnp.dot(x_ref[rows, :], wraw[5], preferred_element_type=F32)
            gt[rows, :] = sigmoid(g)

    for t in range(2):
        for q in range(ROWS):
            rows = [((2 * t + ph) * ROWS + q) * WIDE for ph in range(2)]
            zs[0, q, t] = jnp.concatenate(
                [fac0[pl.ds(first, WIDE), :] for first in rows], axis=0
            ).astype(BF16)
        rows = [pl.multiple_of(((2 * t + ph) * ROWS + y) * WIDE, 8) for ph in range(2)]
        yb[0, y, t] = jnp.concatenate(
            [fac0[pl.ds(first, WIDE), :] for first in rows], axis=0
        ).astype(BF16)
    pl.semaphore_wait(barrier, ROWS - 1 + len(steps))
    for o in (2, 1, 3):
        y_copy(0, 0, o).start()

    project(0)
    over_row(0, 1)
    over_row(0, 2)
    over_col(0, 0)
    over_row(0, 3)
    project(1)
    over_col(0, 1)
    over_row(1, 0)
    over_row(1, 1)
    over_col(0, 2)
    over_row(1, 2)
    over_row(1, 3)
    over_row(1, 4)
    over_col(0, 3)
    over_col(1, 0)
    over_col(1, 1)

    over_col(1, 2)

    for way in (0, 1):
        for r in range(TEAM - 1):
            x_copy(way, r, 0).start()
    gates()
    for near in DIRECT:
        arrived(zb.at[0, pl.ds(0, 2 * len(near))], zrecv.at[(near[-1] - 1) // 2])
        for s in near:
            for way in (0, 1):
                x_copy(way, 0, s).start()
    over_col(1, 3)
    for r in range(1, TEAM - 1):
        for n, group in enumerate(GROUPS[r - 1]):
            arrived(zb.at[0, pl.ds(0, 2 * len(group))], xrecv.at[XBASE[r - 1] + n])
            for s in group:
                for way in (0, 1):
                    x_copy(way, r, s + 1).start()
    over_col(1, 4)

    def near_blocks(half):
        arrived(zb.at[0, pl.ds(0, 2 * sum(s > 0 for s in HALVES[half]))], zrecv.at[3 + half])
        for way in (0, 1):
            for n in range(0, len(HALVES[half]), 2):
                one = rb[way, HALVES[half][n]].astype(F32)
                two = rb[way, HALVES[half][min(n + 1, len(HALVES[half]) - 1)]].astype(F32)
                for ph in (0, 1):
                    cut = slice(WIDE * ph, WIDE * ph + WIDE)
                    rm[way, ph, pl.ds(96 * half + WIDE * n, CHUNK), :] = jnp.concatenate(
                        [one[cut], two[cut]], axis=0
                    ).astype(BF16)

    def left_lines(e):
        for q in range(ROWS):
            four = [lb[e, 4 * q + n].astype(F32) for n in range(4)]
            for ph in (0, 1):
                cut = slice(WIDE * ph, WIDE * ph + WIDE)
                lines = jnp.concatenate([f[cut] for f in four], axis=0).astype(BF16)
                for u in range(3):
                    lm[e, ph, pl.ds(128 * u + 32 * ((q + u) % 4), 32), :] = lines[
                        32 * u : 32 * u + 32
                    ]

    def c_copy(s, way):
        t = 2 * (FAR - s) + way
        return pltpu.make_async_remote_copy(
            src_ref=cs.at[t],
            dst_ref=cb.at[t],
            send_sem=sent.at[3],
            recv_sem=crecv.at[s - 1],
            device_id={"col": col_at(-s if way == 0 else s)},
            device_id_type=MESH,
        )

    scale = (ROWS * LINES) ** -0.5
    for e in range(1, TEAM - 1):
        left_lines(e)
        own = ri[e - 1].astype(F32)
        sums = [
            nt(own[WIDE * ph : WIDE * ph + WIDE].astype(BF16), lm[e, ph]) * scale for ph in (0, 1)
        ]
        cb[2 * FAR + e] = jnp.concatenate(sums, axis=0).astype(BF16)
    near_blocks(0)
    arrived(zb, xrecv.at[XBASE[TEAM - 2]])
    for way in (0, 1):
        left_lines((TEAM - 1) * way)

    for half in (0, 1):
        if half:
            near_blocks(1)
        count = len(HALVES[half])
        for way in (0, 1):
            e = (TEAM - 1) * way
            rows = pl.ds(96 * half, WIDE * count)
            sums = [nt(rm[way, ph, rows, :], lm[e, ph]) * scale for ph in (0, 1)]
            for n, s in enumerate(HALVES[half]):
                cut = slice(WIDE * n, WIDE * n + WIDE)
                chunk = jnp.concatenate([sums[0][cut], sums[1][cut]], axis=0).astype(BF16)
                if s == 0:
                    cb[2 * FAR + e] = chunk
                else:
                    cs[2 * (FAR - s) + way] = chunk
        for s in HALVES[half]:
            for way in (0, 1):
                if s:
                    c_copy(s, way).start()

    def e_copy(sub, o):
        t0, t1 = ESUBS[sub]
        dest = row_at(o)
        return pltpu.make_async_remote_copy(
            src_ref=es.at[dest, pl.ds(t0, t1 - t0)],
            dst_ref=ds.at[y, pl.ds(t0, t1 - t0)],
            send_sem=sent.at[4],
            recv_sem=erecv.at[sub],
            device_id={"row": dest},
            device_id_type=MESH,
        )

    strip = lane // 32

    for sub, (t0, t1) in enumerate(ESUBS):
        if t0 < 2 * FAR:
            arrived(zb.at[0, pl.ds(0, 2)], crecv.at[FAR - t0 // 2 - 1])

        @pl.loop(t0, t1)
        def _(t):
            a, b, c = (cb[t, :, pl.ds(128 * u, 128)].astype(F32) for u in range(3))

            def quarter(q):
                return jnp.where(
                    strip == q, a, jnp.where(strip == lax.rem(q + 1, 4), b, c)
                ).astype(BF16)

            for q in range(ROWS):
                es[q, t] = quarter(q)
            ds[y, t] = quarter(y)

        for o in (2, 1, 3):
            e_copy(sub, o).start()

    mixed = facl
    total = jnp.zeros((WIDE, CH), F32)
    for sub, (t0, t1) in enumerate(ESUBS):
        arrived(ds.at[pl.ds(0, 3), pl.ds(t0, t1 - t0)], erecv.at[sub])

        def add(t, total, t0=t0):
            team = team_of(t, t0 >= 2 * FAR)
            for q in range(ROWS):
                block = ds[q, t].astype(F32)
                first = pl.multiple_of((32 * q + 2 * team) * WIDE, 16)
                mixed[pl.ds(first, CHUNK), :] = block
                total = total + block[:WIDE] + block[WIDE:]
            return total

        total = lax.fori_loop(t0, t1, add, total)
    mean = total * (1.0 / CH)

    def spread(n, total):
        for m in range(8):
            off = mixed[pl.ds(pl.multiple_of((8 * n + m) * WIDE, 8), WIDE), :] - mean
            total = total + off * off
        return total

    var = lax.fori_loop(0, CH // 8, spread, jnp.zeros((WIDE, CH), F32)) * (1.0 / CH)
    stat[0] = mean
    stat[1] = lax.rsqrt(var + 1e-05)

    out = facr

    @pl.loop(0, WIDE // 4, unroll=2)
    def _(n):
        scaled = []
        for j in range(4):
            block = mixed[pl.ds(4 * n + j, CH, stride=WIDE), :]
            block = (block - stat[0, pl.ds(4 * n + j, 1), :]) * stat[1, pl.ds(4 * n + j, 1), :] * gb[...]
            scaled.append(block.astype(BF16).T)
        change = jnp.dot(jnp.concatenate(scaled, axis=0), wraw[4], preferred_element_type=F32)
        for j in range(4):
            for b in range(4):
                u = lax.rem(b - y + 4, 4)
                out[pl.ds(u * (32 * WIDE) + 4 * n + j, 32, stride=WIDE), :] = change[
                    CH * j + 32 * b : CH * j + 32 * b + 32
                ]

    @pl.loop(0, 6)
    def _(n):
        rows = pl.ds(pl.multiple_of(n * 384, 384), 384)
        o_ref[rows, :] = (out[rows, :] * gt[rows, :]).astype(BF16)

    departed(zs.at[:, pl.ds(0, 3)], sent.at[0])
    departed(zb, sent.at[1])
    departed(lb.at[pl.ds(0, TEAM - 1)], sent.at[2])
    departed(cs, sent.at[3])
    departed(es.at[pl.ds(0, 3)], sent.at[4])


def per_device(
    pair_rows, left_weight, right_weight, left_gate, right_gate, mid_gain, out_weight, out_gate
):
    pixels = pair_rows.shape[0] * pair_rows.shape[1]
    dma = pltpu.SemaphoreType.DMA
    out = pl.pallas_call(
        kernel,
        out_shape=jax.ShapeDtypeStruct((pixels, CH), BF16),
        in_specs=[pl.BlockSpec(memory_space=pltpu.HBM)] * 8,
        out_specs=pl.BlockSpec(memory_space=pltpu.VMEM),
        scratch_shapes=[
            pltpu.VMEM((pixels, CH), BF16),
            pltpu.VMEM((6, CH, CH), BF16),
            pltpu.VMEM((1, CH), F32),
            pltpu.VMEM((128 * WIDE, CH), F32),
            pltpu.VMEM((128 * WIDE, CH), BF16),
            pltpu.VMEM((2 * CH, CH), F32),
            pltpu.VMEM((4 * CH, CH), BF16),
            pltpu.VMEM((CH, CH), F32),
            pltpu.VMEM((CH * WIDE, CH), F32),
            pltpu.VMEM((CH * WIDE, CH), F32),
            pltpu.VMEM((16 * WIDE, CH), F32),
            pltpu.VMEM((2, ROWS, COLS, CHUNK, CH), BF16),
            pltpu.VMEM((2, ROWS, COLS, CHUNK, CH), BF16),
            pltpu.VMEM((2, 2 * FAR, CHUNK, 384), BF16),
            pltpu.VMEM((TEAM, COLS, CHUNK, 384), BF16),
            pltpu.VMEM((2, FAR + 1, CHUNK, 384), BF16),
            pltpu.VMEM((TEAM - 2, CHUNK, 384), BF16),
            pltpu.VMEM((TEAM, 2, 384, 384), BF16),
            pltpu.VMEM((2, 2, 192, 384), BF16),
            pltpu.VMEM((2 * FAR, CHUNK, 384), BF16),
            pltpu.VMEM((COLS, CHUNK, 384), BF16),
            pltpu.VMEM((ROWS, COLS, CHUNK, CH), BF16),
            pltpu.VMEM((ROWS, COLS, CHUNK, CH), BF16),
            pltpu.VMEM((pixels, CH), F32),
            pltpu.VMEM((2, WIDE, CH), F32),
            dma((3,)), dma((5,)), dma((9,)), dma((5,)), dma((XBASE[-1],)), dma((FAR,)), dma((len(ESUBS),)),
        ],
        compiler_params=pltpu.CompilerParams(
            collective_id=0, has_side_effects=True, vmem_limit_bytes=48 * 1024 * 1024
        ),
    )(
        *[
            pltpu.with_memory_space_constraint(v, pltpu.HBM)
            for v in (
                pair_rows.reshape(pixels, CH),
                left_weight, left_gate, right_weight, right_gate,
                mid_gain.reshape(1, CH), out_weight, out_gate,
            )
        ]
    )
    return out.reshape(pair_rows.shape)


def solution(mesh):
    placed = (
        P(("trial", "row"), "col", None),
        P("trial", None),
        P("trial", None),
        P("trial", None),
        P("trial", None),
        P(),
        P("trial", None),
        P("trial", None),
    )
    return jax.shard_map(
        per_device,
        mesh=mesh,
        in_specs=placed,
        out_specs=P(("trial", "row"), "col", None),
        check_vma=False,
    )
```

```python
import functools

import jax
import jax.numpy as jnp
from jax import lax
from jax.experimental import pallas as pl
from jax.experimental.pallas import tpu as pltpu
from jax.sharding import PartitionSpec as P

MESH = pl.DeviceIdType.MESH
F32, BF16 = jnp.float32, jnp.bfloat16
ROWS, COLS = 4, 16
LINES, WIDE, CH = 96, 24, 128
TEAM = 6
FAR = (COLS - TEAM) // 2
CHUNK = 2 * WIDE
YSUBS = (((0, 2), (2, 6), (6, 10), (10, 16)), ((10, 16), (0, 2), (2, 4), (4, 6), (6, 10)))
ESUBS = ((10, 16), (0, 2), (2, 4), (4, 6), (6, 8), (8, 10))
HALVES = ((0, 5, 4, 3), (2, 1))
DIRECT = ((5,), (4, 3), (2, 1))
ORDERS = [[0, 5, 4, 3, 2, 1]]
while len(ORDERS) < TEAM - 1:
    ORDERS.append([0] + [s + 1 for s in ORDERS[-1]])
GROUPS = [[order[n : n + 2] for n in range(0, len(order), 2)] for order in ORDERS]
GROUPS[-1] = [ORDERS[-1]]
XBASE = [sum(len(g) for g in GROUPS[:r]) for r in range(TEAM)]


def hand_sem(r, s):
    return XBASE[r] + [s in group for group in GROUPS[r]].index(True)


def sigmoid(x):
    return 0.5 + 0.5 * jnp.tanh(0.5 * x)


def nt(a, b):
    return lax.dot_general(a, b, (((1,), (1,)), ((), ())), preferred_element_type=F32)


def kernel(
    x_hbm, lw_hbm, lg_hbm, rw_hbm, rg_hbm, gain_hbm, ow_hbm, og_hbm,
    o_ref,
    x_ref, wraw, gain_ref, xf, xr, wf, wt, gb, facl, facr, fac0, zs, yb, zb, lb, rb, ri, lm, rm,
    cs, cb, es, ds, gt, stat,
    insem, sent, yrecv, zrecv, xrecv, crecv, erecv,
):
    y = lax.axis_index("row")
    z = lax.axis_index("col")

    def row_at(o):
        return lax.rem(y + o, ROWS)

    def col_at(s):
        return lax.rem(z + s + COLS, COLS)

    steps = [(s, way) for s in range(FAR, 0, -1) for way in (0, 1)]

    mats = (lw_hbm, lg_hbm, rw_hbm, rg_hbm, ow_hbm, og_hbm)
    loads = [pltpu.make_async_copy(m, wraw.at[n], insem.at[0]) for n, m in enumerate(mats)]
    loads += [pltpu.make_async_copy(gain_hbm, gain_ref, insem.at[1])]
    loads += [pltpu.make_async_copy(x_hbm, x_ref, insem.at[2])]
    for load in loads:
        load.start()

    def arrived(ref, sem):
        pltpu.make_async_remote_copy(
            src_ref=ref, dst_ref=ref, send_sem=sem, recv_sem=sem,
            device_id={"col": col_at(1)}, device_id_type=MESH,
        ).wait_recv()

    def departed(ref, sem):
        pltpu.make_async_remote_copy(
            src_ref=ref, dst_ref=ref, send_sem=sem, recv_sem=sem,
            device_id={"col": col_at(1)}, device_id_type=MESH,
        ).wait_send()

    barrier = pltpu.get_barrier_semaphore()
    for o in range(1, ROWS):
        pl.semaphore_signal(barrier, inc=1, device_id={"row": row_at(o)}, device_id_type=MESH)
    for s, way in steps:
        pl.semaphore_signal(
            barrier, inc=1, device_id={"col": col_at(s if way == 0 else -s)}, device_id_type=MESH
        )

    def team_of(t, own):
        if own:
            return lax.rem(z + COLS - (t - 2 * FAR), COLS)
        s = FAR - t // 2
        way = t % 2
        return lax.rem(z + COLS + (1 - 2 * way) * s - (TEAM - 1) * way, COLS)

    facs = (facl, facr)

    xf[pl.ds(LINES * WIDE, 32 * WIDE), :] = jnp.zeros((32 * WIDE, CH), F32)
    pltpu.make_async_copy(wraw, wraw, insem.at[0]).wait()
    loads[6].wait()
    for n in range(4):
        turned = wraw[n].astype(F32).T
        if n < 2:
            wf[pl.ds(CH * n, CH), :] = turned
        wt[pl.ds(CH * n, CH), :] = turned.astype(BF16)
    gb[...] = jnp.broadcast_to(gain_ref[...], (CH, CH)).T
    picks = []
    for n in range(2):
        for t in range(2):
            for ph in range(2):
                picks.append(wf[pl.ds(CH * n + 2 * team_of(t, False) + ph, ROWS, stride=32), :])
    first_w = jnp.concatenate(picks, axis=0).astype(BF16)
    loads[7].wait()
    xf[pl.ds(0, LINES * WIDE), :] = x_ref[...].astype(F32)

    @pl.loop(0, WIDE // 2, unroll=6)
    def _(n):
        parts = []
        for i in (2 * n, 2 * n + 1):
            for b in range(4):
                block = lax.rem(b + y, 4)
                parts.append(xf[pl.ds(block * (32 * WIDE) + i, 32, stride=WIDE), :])
        xi = jnp.concatenate(parts, axis=0).astype(BF16)
        xr[pl.ds(pl.multiple_of(2 * CH * n, 2 * CH), 2 * CH), :] = xi
        both = nt(first_w, xi)
        value = both[:16] * sigmoid(both[16:])
        for m in range(2):
            fac0[pl.ds(2 * n + m, 16, stride=WIDE), :] = value[:, CH * m : CH * m + CH]

    def project(arr):
        @pl.loop(0, WIDE // 2, unroll=6)
        def _(n):
            xi = xr[pl.ds(pl.multiple_of(2 * CH * n, 2 * CH), 2 * CH), :]
            both = nt(wt[pl.ds(2 * CH * arr, 2 * CH), :], xi)
            value = both[:CH] * sigmoid(both[CH:])
            for m in range(2):
                facs[arr][pl.ds(2 * n + m, CH, stride=WIDE), :] = value[:, CH * m : CH * m + CH]

    def y_copy(arr, sub, o):
        t0, t1 = YSUBS[arr][sub]
        dest = row_at(o)
        return pltpu.make_async_remote_copy(
            src_ref=zs.at[arr, dest, pl.ds(t0, t1 - t0)],
            dst_ref=yb.at[arr, y, pl.ds(t0, t1 - t0)],
            send_sem=sent.at[0],
            recv_sem=yrecv.at[4 * arr + sub],
            device_id={"row": dest},
            device_id_type=MESH,
        )

    def over_row(arr, sub):
        t0, t1 = YSUBS[arr][sub]

        @pl.loop(t0, t1)
        def _(t):
            team = team_of(t, t0 >= 2 * FAR)
            for q in range(ROWS):
                first = pl.multiple_of((32 * q + 2 * team) * WIDE, 16)
                zs[arr, q, t] = facs[arr][pl.ds(first, CHUNK), :].astype(BF16)
            first = pl.multiple_of((32 * y + 2 * team) * WIDE, 16)
            yb[arr, y, t] = facs[arr][pl.ds(first, CHUNK), :].astype(BF16)

        for o in (2, 1, 3):
            y_copy(arr, sub, o).start()

    def z_copy(arr, s, way):
        t = 2 * (FAR - s) + way
        dst = lb.at[(TEAM - 1) * way, z] if arr == 0 else rb.at[way, s]
        return pltpu.make_async_remote_copy(
            src_ref=zb.at[arr, t],
            dst_ref=dst,
            send_sem=sent.at[1],
            recv_sem=zrecv.at[(s - 1) // 2 if arr == 0 else 3 if s in HALVES[0] else 4],
            device_id={"col": col_at(s if way == 0 else -s)},
            device_id_type=MESH,
        )

    lane = lax.broadcasted_iota(jnp.int32, (CHUNK, CH), 1)

    def join(arr, t):
        a, b, c, d = (yb[arr, q, t].astype(F32) for q in range(ROWS))
        return jnp.concatenate(
            [
                jnp.where(lane < 96, a, b),
                jnp.where(lane < 64, b, c),
                jnp.where(lane < 32, c, d),
            ],
            axis=1,
        ).astype(BF16)

    def over_col(arr, sub):
        t0, t1 = YSUBS[arr][sub]
        arrived(yb.at[arr, pl.ds(0, 3), pl.ds(t0, t1 - t0)], yrecv.at[4 * arr + sub])
        if t0 >= 2 * FAR:
            for e in range(TEAM):
                if arr == 0:
                    lb[e, z] = join(arr, t0 + e)
                elif e in (0, TEAM - 1):
                    rb[e // (TEAM - 1), 0] = join(arr, t0 + e)
                else:
                    ri[e - 1] = join(arr, t0 + e)
            return

        @pl.loop(t0, t1)
        def _(t):
            zb[arr, t] = join(arr, t)

        for t in range(t0, t1):
            z_copy(arr, FAR - t // 2, t % 2).start()

    def x_copy(way, r, s):
        src = col_at(-s if way == 0 else s)
        e = r if way == 0 else TEAM - 1 - r
        return pltpu.make_async_remote_copy(
            src_ref=lb.at[e, src],
            dst_ref=lb.at[e + 1 - 2 * way, src],
            send_sem=sent.at[2],
            recv_sem=xrecv.at[hand_sem(r, s)],
            device_id={"col": col_at(1 if way == 0 else -1)},
            device_id_type=MESH,
        )

    def gates():
        @pl.loop(0, 6)
        def _(n):
            rows = pl.ds(pl.multiple_of(n * 384, 384), 384)
            g = jnp.dot(x_ref[rows, :], wraw[5], preferred_element_type=F32)
            gt[rows, :] = sigmoid(g)

    for t in range(2):
        for q in range(ROWS):
            rows = [((2 * t + ph) * ROWS + q) * WIDE for ph in range(2)]
            zs[0, q, t] = jnp.concatenate(
                [fac0[pl.ds(first, WIDE), :] for first in rows], axis=0
            ).astype(BF16)
        rows = [pl.multiple_of(((2 * t + ph) * ROWS + y) * WIDE, 8) for ph in range(2)]
        yb[0, y, t] = jnp.concatenate(
            [fac0[pl.ds(first, WIDE), :] for first in rows], axis=0
        ).astype(BF16)
    pl.semaphore_wait(barrier, ROWS - 1 + len(steps))
    for o in (2, 1, 3):
        y_copy(0, 0, o).start()

    project(0)
    over_row(0, 1)
    over_row(0, 2)
    over_col(0, 0)
    over_row(0, 3)
    project(1)
    over_col(0, 1)
    over_row(1, 0)
    over_row(1, 1)
    over_col(0, 2)
    over_row(1, 2)
    over_row(1, 3)
    over_row(1, 4)
    over_col(0, 3)
    over_col(1, 0)
    over_col(1, 1)

    over_col(1, 2)

    for way in (0, 1):
        for r in range(TEAM - 1):
            x_copy(way, r, 0).start()
    gates()
    for near in DIRECT:
        arrived(zb.at[0, pl.ds(0, 2 * len(near))], zrecv.at[(near[-1] - 1) // 2])
        for s in near:
            for way in (0, 1):
                x_copy(way, 0, s).start()
    over_col(1, 3)
    for r in range(1, TEAM - 1):
        for n, group in enumerate(GROUPS[r - 1]):
            arrived(zb.at[0, pl.ds(0, 2 * len(group))], xrecv.at[XBASE[r - 1] + n])
            for s in group:
                for way in (0, 1):
                    x_copy(way, r, s + 1).start()
    over_col(1, 4)

    def near_blocks(half):
        arrived(zb.at[0, pl.ds(0, 2 * sum(s > 0 for s in HALVES[half]))], zrecv.at[3 + half])
        for way in (0, 1):
            for n in range(0, len(HALVES[half]), 2):
                one = rb[way, HALVES[half][n]].astype(F32)
                two = rb[way, HALVES[half][min(n + 1, len(HALVES[half]) - 1)]].astype(F32)
                for ph in (0, 1):
                    cut = slice(WIDE * ph, WIDE * ph + WIDE)
                    rm[way, ph, pl.ds(96 * half + WIDE * n, CHUNK), :] = jnp.concatenate(
                        [one[cut], two[cut]], axis=0
                    ).astype(BF16)

    def left_lines(e):
        for q in range(ROWS):
            four = [lb[e, 4 * q + n].astype(F32) for n in range(4)]
            for ph in (0, 1):
                cut = slice(WIDE * ph, WIDE * ph + WIDE)
                lines = jnp.concatenate([f[cut] for f in four], axis=0).astype(BF16)
                for u in range(3):
                    lm[e, ph, pl.ds(128 * u + 32 * ((q + u) % 4), 32), :] = lines[
                        32 * u : 32 * u + 32
                    ]

    def c_copy(s, way):
        t = 2 * (FAR - s) + way
        return pltpu.make_async_remote_copy(
            src_ref=cs.at[t],
            dst_ref=cb.at[t],
            send_sem=sent.at[3],
            recv_sem=crecv.at[s - 1],
            device_id={"col": col_at(-s if way == 0 else s)},
            device_id_type=MESH,
        )

    scale = (ROWS * LINES) ** -0.5
    for e in range(1, TEAM - 1):
        left_lines(e)
        own = ri[e - 1].astype(F32)
        sums = [
            nt(own[WIDE * ph : WIDE * ph + WIDE].astype(BF16), lm[e, ph]) * scale for ph in (0, 1)
        ]
        cb[2 * FAR + e] = jnp.concatenate(sums, axis=0).astype(BF16)
    near_blocks(0)
    arrived(zb, xrecv.at[XBASE[TEAM - 2]])
    for way in (0, 1):
        left_lines((TEAM - 1) * way)

    for half in (0, 1):
        if half:
            near_blocks(1)
        count = len(HALVES[half])
        for way in (0, 1):
            e = (TEAM - 1) * way
            rows = pl.ds(96 * half, WIDE * count)
            sums = [nt(rm[way, ph, rows, :], lm[e, ph]) * scale for ph in (0, 1)]
            for n, s in enumerate(HALVES[half]):
                cut = slice(WIDE * n, WIDE * n + WIDE)
                chunk = jnp.concatenate([sums[0][cut], sums[1][cut]], axis=0).astype(BF16)
                if s == 0:
                    cb[2 * FAR + e] = chunk
                else:
                    cs[2 * (FAR - s) + way] = chunk
        for s in HALVES[half]:
            for way in (0, 1):
                if s:
                    c_copy(s, way).start()

    def e_copy(sub, o):
        t0, t1 = ESUBS[sub]
        dest = row_at(o)
        return pltpu.make_async_remote_copy(
            src_ref=es.at[dest, pl.ds(t0, t1 - t0)],
            dst_ref=ds.at[y, pl.ds(t0, t1 - t0)],
            send_sem=sent.at[4],
            recv_sem=erecv.at[sub],
            device_id={"row": dest},
            device_id_type=MESH,
        )

    strip = lane // 32

    for sub, (t0, t1) in enumerate(ESUBS):
        if t0 < 2 * FAR:
            arrived(zb.at[0, pl.ds(0, 2)], crecv.at[FAR - t0 // 2 - 1])

        @pl.loop(t0, t1)
        def _(t):
            a, b, c = (cb[t, :, pl.ds(128 * u, 128)].astype(F32) for u in range(3))

            def quarter(q):
                return jnp.where(
                    strip == q, a, jnp.where(strip == lax.rem(q + 1, 4), b, c)
                ).astype(BF16)

            for q in range(ROWS):
                es[q, t] = quarter(q)
            ds[y, t] = quarter(y)

        for o in (2, 1, 3):
            e_copy(sub, o).start()

    mixed = facl
    total = jnp.zeros((WIDE, CH), F32)
    for sub, (t0, t1) in enumerate(ESUBS):
        arrived(ds.at[pl.ds(0, 3), pl.ds(t0, t1 - t0)], erecv.at[sub])

        def add(t, total, t0=t0):
            team = team_of(t, t0 >= 2 * FAR)
            for q in range(ROWS):
                block = ds[q, t].astype(F32)
                first = pl.multiple_of((32 * q + 2 * team) * WIDE, 16)
                mixed[pl.ds(first, CHUNK), :] = block
                total = total + block[:WIDE] + block[WIDE:]
            return total

        total = lax.fori_loop(t0, t1, add, total, unroll=2)
    mean = total * (1.0 / CH)

    def spread(n, total):
        for m in range(8):
            off = mixed[pl.ds(pl.multiple_of((8 * n + m) * WIDE, 8), WIDE), :] - mean
            total = total + off * off
        return total

    var = lax.fori_loop(0, CH // 8, spread, jnp.zeros((WIDE, CH), F32), unroll=2) * (1.0 / CH)
    stat[0] = mean
    stat[1] = lax.rsqrt(var + 1e-05)

    out = facr

    @pl.loop(0, WIDE // 4, unroll=6)
    def _(n):
        scaled = []
        for j in range(4):
            block = mixed[pl.ds(4 * n + j, CH, stride=WIDE), :]
            block = (block - stat[0, pl.ds(4 * n + j, 1), :]) * stat[1, pl.ds(4 * n + j, 1), :] * gb[...]
            scaled.append(block.astype(BF16).T)
        change = jnp.dot(jnp.concatenate(scaled, axis=0), wraw[4], preferred_element_type=F32)
        for j in range(4):
            for b in range(4):
                u = lax.rem(b - y + 4, 4)
                out[pl.ds(u * (32 * WIDE) + 4 * n + j, 32, stride=WIDE), :] = change[
                    CH * j + 32 * b : CH * j + 32 * b + 32
                ]

    @pl.loop(0, 6, unroll=2)
    def _(n):
        rows = pl.ds(pl.multiple_of(n * 384, 384), 384)
        o_ref[rows, :] = (out[rows, :] * gt[rows, :]).astype(BF16)

    departed(zs.at[:, pl.ds(0, 3)], sent.at[0])
    departed(zb, sent.at[1])
    departed(lb.at[pl.ds(0, TEAM - 1)], sent.at[2])
    departed(cs, sent.at[3])
    departed(es.at[pl.ds(0, 3)], sent.at[4])


def per_device(
    pair_rows, left_weight, right_weight, left_gate, right_gate, mid_gain, out_weight, out_gate
):
    pixels = pair_rows.shape[0] * pair_rows.shape[1]
    dma = pltpu.SemaphoreType.DMA
    out = pl.pallas_call(
        kernel,
        out_shape=jax.ShapeDtypeStruct((pixels, CH), BF16),
        in_specs=[pl.BlockSpec(memory_space=pltpu.HBM)] * 8,
        out_specs=pl.BlockSpec(memory_space=pltpu.VMEM),
        scratch_shapes=[
            pltpu.VMEM((pixels, CH), BF16),
            pltpu.VMEM((6, CH, CH), BF16),
            pltpu.VMEM((1, CH), F32),
            pltpu.VMEM((128 * WIDE, CH), F32),
            pltpu.VMEM((128 * WIDE, CH), BF16),
            pltpu.VMEM((2 * CH, CH), F32),
            pltpu.VMEM((4 * CH, CH), BF16),
            pltpu.VMEM((CH, CH), F32),
            pltpu.VMEM((CH * WIDE, CH), F32),
            pltpu.VMEM((CH * WIDE, CH), F32),
            pltpu.VMEM((16 * WIDE, CH), F32),
            pltpu.VMEM((2, ROWS, COLS, CHUNK, CH), BF16),
            pltpu.VMEM((2, ROWS, COLS, CHUNK, CH), BF16),
            pltpu.VMEM((2, 2 * FAR, CHUNK, 384), BF16),
            pltpu.VMEM((TEAM, COLS, CHUNK, 384), BF16),
            pltpu.VMEM((2, FAR + 1, CHUNK, 384), BF16),
            pltpu.VMEM((TEAM - 2, CHUNK, 384), BF16),
            pltpu.VMEM((TEAM, 2, 384, 384), BF16),
            pltpu.VMEM((2, 2, 192, 384), BF16),
            pltpu.VMEM((2 * FAR, CHUNK, 384), BF16),
            pltpu.VMEM((COLS, CHUNK, 384), BF16),
            pltpu.VMEM((ROWS, COLS, CHUNK, CH), BF16),
            pltpu.VMEM((ROWS, COLS, CHUNK, CH), BF16),
            pltpu.VMEM((pixels, CH), F32),
            pltpu.VMEM((2, WIDE, CH), F32),
            dma((3,)), dma((5,)), dma((9,)), dma((5,)), dma((XBASE[-1],)), dma((FAR,)), dma((len(ESUBS),)),
        ],
        compiler_params=pltpu.CompilerParams(
            collective_id=0, has_side_effects=True, vmem_limit_bytes=48 * 1024 * 1024
        ),
    )(
        *[
            pltpu.with_memory_space_constraint(v, pltpu.HBM)
            for v in (
                pair_rows.reshape(pixels, CH),
                left_weight, left_gate, right_weight, right_gate,
                mid_gain.reshape(1, CH), out_weight, out_gate,
            )
        ]
    )
    return out.reshape(pair_rows.shape)


def solution(mesh):
    placed = (
        P(("trial", "row"), "col", None),
        P("trial", None),
        P("trial", None),
        P("trial", None),
        P("trial", None),
        P(),
        P("trial", None),
        P("trial", None),
    )
    return jax.shard_map(
        per_device,
        mesh=mesh,
        in_specs=placed,
        out_specs=P(("trial", "row"), "col", None),
        check_vma=False,
    )
```
